32 devices in a mesh: groups: 2 (over y), batch: 8 (over z, x), mp: 2 (over core).
Axes of the slice: x: 2, y: 2, z: 4, core: 2. Of those that a mesh axis runs over, the one named last changes fastest.
Arguments:
- hidden: bfloat16 [32, 1280], P(('groups', 'batch')), parts along dimension 0, may hold values from -6 to 6
- token_qkv: bfloat16 [3, 32, 1280], P(None, ('groups', 'batch'), 'mp'), parts along dimension 1, may hold values from -6 to 6
- self_cache: bfloat16 [2, 32, 128, 1280], P(None, ('groups', 'batch'), None, 'mp'), parts along dimension 1, may hold values from -6 to 6
- cross_kv: bfloat16 [2, 32, 64, 1280], P(None, ('groups', 'batch'), None, 'mp'), parts along dimension 1, may hold values from -6 to 6
- cache_len: int32 [32], P(('groups', 'batch')), parts along dimension 0, may hold values from 1 to 127
- finished: int32 [32], P(('groups', 'batch')), parts along dimension 0, may hold values 0 or 1
- new_slot: int32 [32], P(('groups', 'batch')), parts along dimension 0, may hold values from 0 to 15, as said below
- out_proj: bfloat16 [1280, 1280], P('mp'), may hold values from -0.15625 to 0.15625
- ln_gain: float32 [1280], replicated, may hold values from 0.5 to 1.5
- ln_bias: float32 [1280], replicated, may hold values from -3 to 3
- query_proj: bfloat16 [1280, 1280], P(None, 'mp'), may hold values from -3 to 3
Outputs:
- moved_cache: bfloat16 [2, 32, 128, 1280], P(None, ('groups', 'batch'), None, 'mp'), parts along dimension 1
- moved_out: bfloat16 [32, 1280], P(('groups', 'batch'), 'mp'), parts along dimension 0
The draws below stay inside these ranges and needn't reach their ends.
There are 2 independent parts, one for each index of `groups`. The reference program is written for one: setup_inputs(seed, part) draws one part's arguments, and reference() takes and returns one part's arrays. A program takes and returns all parts, laid end to end along the dimension named above; an argument that names none is the same for every part. Nothing has to cross between parts.
Inputs may be any that keep to these rules, and one draw needn't show every extreme that they name: A permutation of the spans' slots. Span c's new owner new_slot[c] // 2 lies within 3 devices of its present one c // 2, counting the device order as a loop; of one device's spans at most one moves by any given signed distance.
All inputs are finite; a program needn't handle non-finite values. No bound on the sum of `finished` on one device may be relied on, other than what follows from the above.
Results may differ from the reference program's by a relative error of at most 0.015.
Values may be sent and summed in bfloat16 or wider, within the bound.
A program may use at most 64 MiB of HBM per device.

```python
import jax
import jax.numpy as jnp
from jax import lax

D = 1280
HEADS = 20
HEAD_DIM = 64
CH_DEV = 2
ENC = 64
SLOTS = 128
SPANS = 16


def swap_round(key, table, stride, period):
    devices, width = table.shape
    keys = jax.random.split(key, 4)
    phase = jax.random.randint(keys[0], (), 0, period)
    left_slot = jax.random.randint(keys[1], (devices,), 0, width)
    right_slot = jax.random.randint(keys[2], (devices,), 0, width)
    coin = jax.random.randint(keys[3], (devices,), 0, 2)
    index = jnp.arange(devices, dtype=jnp.int32)
    is_left = (index - phase) % period < stride
    partner = jnp.where(is_left, (index + stride) % devices, (index - stride) % devices)
    leader = jnp.where(is_left, index, partner)
    mine = jnp.where(is_left, left_slot[leader], right_slot[leader])
    theirs = jnp.where(is_left, right_slot[leader], left_slot[leader])
    swapping = coin[leader] == 1
    incoming = table[partner, theirs]
    column = jnp.arange(width, dtype=jnp.int32)[None, :] == mine[:, None]
    return jnp.where(column & swapping[:, None], incoming[:, None], table)


def draw_new_slot(key, part):
    devices = SPANS // CH_DEV
    table = jnp.arange(SPANS, dtype=jnp.int32).reshape(devices, CH_DEV)
    table = swap_round(jax.random.fold_in(key, 11), table, 1, 2)
    table = swap_round(jax.random.fold_in(key, 12), table, 2, 4)
    return jnp.zeros((SPANS,), jnp.int32).at[table.reshape(-1)].set(jnp.arange(SPANS, dtype=jnp.int32))


def rough_noise(key, shape):
    return jax.random.truncated_normal(key, -6.0, 6.0, shape, jnp.float32)


def fixed_pattern():
    dims = jnp.arange(HEAD_DIM, dtype=jnp.int32)
    return jnp.where((dims * 37 + 11) % 8 < 4, 1.0, -1.0).astype(jnp.float32)


def self_plan(key):
    keys = jax.random.split(jax.random.fold_in(key, 71), 7)
    span_index = jnp.arange(SPANS, dtype=jnp.int32)[:, None]
    head_index = jnp.arange(HEADS, dtype=jnp.int32)[None, :]
    first_span = jax.random.randint(keys[0], (), 0, SPANS)
    first_head = jax.random.randint(keys[1], (), 0, HEADS)
    forced = (span_index == first_span) & (head_index == first_head)
    planted = (jax.random.randint(keys[2], (SPANS, HEADS), 0, 16) == 0) | forced
    signs = (2 * jax.random.randint(keys[3], (SPANS, HEADS, HEAD_DIM), 0, 2) - 1).astype(jnp.float32)
    query_steps = jnp.where(forced, 185, jax.random.randint(keys[4], (SPANS, HEADS), 112, 186))
    key_steps = jnp.where(forced, 185, jax.random.randint(keys[5], (SPANS, HEADS), 144, 186))
    own_first = jax.random.randint(keys[6], (SPANS, HEADS), 0, 2) == 1
    higher = key_steps.astype(jnp.float32) / 32.0
    lower = (key_steps - 2).astype(jnp.float32) / 32.0
    query_scale = query_steps.astype(jnp.float32) / 32.0
    own_scale = jnp.where(own_first, higher, lower)
    cached_scale = jnp.where(own_first, lower, higher)
    return (planted, signs, query_scale, own_scale, cached_scale)


def draw_token_qkv(key, part):
    base = rough_noise(jax.random.fold_in(key, 1), (3, SPANS, HEADS, HEAD_DIM))
    planted, signs, query_scale, own_scale, cached_scale = self_plan(key)
    mask = planted[:, :, None]
    query_part = jnp.where(mask, query_scale[:, :, None] * signs, base[0])
    key_part = jnp.where(mask, own_scale[:, :, None] * signs, base[1])
    stacked = jnp.stack([query_part, key_part, base[2]])
    return stacked.reshape(3, SPANS, D).astype(jnp.bfloat16)


def draw_self_cache(key, part):
    base = rough_noise(jax.random.fold_in(key, 2), (2, SPANS, SLOTS, HEADS, HEAD_DIM))
    planted, signs, query_scale, own_scale, cached_scale = self_plan(key)
    first_keys = jnp.where(planted[:, :, None], cached_scale[:, :, None] * signs, base[0, :, 0])
    base = base.at[0, :, 0].set(first_keys)
    return base.reshape(2, SPANS, SLOTS, D).astype(jnp.bfloat16)


def draw_cross_kv(key, part):
    base = rough_noise(jax.random.fold_in(key, 3), (2, SPANS, ENC, HEADS, HEAD_DIM))
    keys = jax.random.split(jax.random.fold_in(key, 73), 5)
    span_index = jnp.arange(SPANS, dtype=jnp.int32)
    forced_span = jax.random.randint(keys[0], (), 0, SPANS)
    planted = (jax.random.randint(keys[1], (SPANS,), 0, 8) == 0) | (span_index == forced_span)
    first_frame = jax.random.randint(keys[2], (SPANS,), 0, ENC)
    second_frame = (first_frame + 1 + jax.random.randint(keys[3], (SPANS,), 0, ENC - 1)) % ENC
    key_steps = jnp.where(span_index == forced_span, 184, jax.random.randint(keys[4], (SPANS,), 96, 186))
    higher = key_steps.astype(jnp.float32) / 32.0
    lower = (key_steps - 2).astype(jnp.float32) / 32.0
    frame = jnp.arange(ENC, dtype=jnp.int32)[None, :]
    at_first = frame == first_frame[:, None]
    at_second = frame == second_frame[:, None]
    scale = jnp.where(at_first, higher[:, None], jnp.where(at_second, lower[:, None], 0.0))
    use = planted[:, None] & (at_first | at_second)
    pattern = fixed_pattern()
    key_part = jnp.where(use[:, :, None, None], scale[:, :, None, None] * pattern[None, None, None, :], base[0])
    stacked = jnp.stack([key_part, base[1]])
    return stacked.reshape(2, SPANS, ENC, D).astype(jnp.bfloat16)


def bias_plan(key):
    keys = jax.random.split(jax.random.fold_in(key, 91), 3)
    bias = 0.5 * jax.random.truncated_normal(keys[0], -6.0, 6.0, (D,), jnp.float32)
    head_index = jnp.arange(HEADS, dtype=jnp.int32)
    chosen_head = jax.random.randint(keys[1], (), 0, HEADS)
    heads_on = (jax.random.randint(keys[2], (HEADS,), 0, 4) == 0) | (head_index == chosen_head)
    return (bias, heads_on)


def draw_ln_bias(key, part):
    bias, heads_on = bias_plan(key)
    return bias


def draw_query_proj(key, part):
    bias, heads_on = bias_plan(key)
    weight_key = jax.random.fold_in(key, 92)
    weight = jax.random.truncated_normal(weight_key, -6.0, 6.0, (D, D), jnp.float32) * D ** (-0.5)
    direction = 5.0 * jnp.where(heads_on[:, None], fixed_pattern()[None, :], 0.0).reshape(D)
    norm_sq = jnp.maximum(jnp.sum(bias * bias), D / 8.0)
    weight = weight + (bias / norm_sq)[:, None] * direction[None, :]
    return weight.astype(jnp.bfloat16)


def set_ends(drawn, own_key, low, high):
    extent = drawn.shape
    place = [jax.random.randint(jax.random.fold_in(own_key, axis), (), 0, extent[axis]) for axis in range(len(extent))]
    drawn = drawn.at[tuple(place)].set(low)
    longest = extent.index(max(extent))
    place[longest] = (place[longest] + 1) % extent[longest]
    return drawn.at[tuple(place)].set(high)


def shard_levels(key, shape, shards, low, top_value):
    factor_of, own = 1.0, jax.random.fold_in(key, 6)
    for dim, shards_of in shards:
        heights = jnp.exp(jax.random.uniform(jax.random.fold_in(own, dim), (shards_of,), jnp.float32, low / len(shards), top_value / len(shards)))
        factor_of = factor_of * jnp.repeat(heights, shape[dim] // shards_of).reshape([-1 if axis == dim else 1 for axis in range(len(shape))])
    return factor_of


def noise(key, extent, deviation, reach, shards=(), kind=jnp.bfloat16):
    values = deviation * jax.random.normal(key, extent, jnp.float32)
    if shards:
        values = values * shard_levels(key, extent, shards, -0.22, 0.18)
    return jnp.clip(values, -reach, reach).astype(kind)


def setup_inputs(seed: int = 0, part: int = 0) -> dict:
    seeds = jax.random.split(jax.random.key(seed), 12)
    part_splits = jax.random.split(jax.random.fold_in(seeds[11], part), 12)
    return {
        "hidden": noise(part_splits[0], (SPANS, D), 1.0, 6.0, ((0, 8),)),
        "token_qkv": draw_token_qkv(jax.random.fold_in(jax.random.fold_in(seeds[11], part), 71), part),
        "self_cache": draw_self_cache(jax.random.fold_in(jax.random.fold_in(seeds[11], part), 71), part),
        "cross_kv": draw_cross_kv(jax.random.fold_in(jax.random.fold_in(seeds[11], part), 71), part),
        "cache_len": set_ends(jax.random.randint(part_splits[4], (SPANS,), 1, SLOTS), jax.random.fold_in(part_splits[4], 1), 1, SLOTS - 1).astype(jnp.int32),
        "finished": set_ends((jax.random.randint(part_splits[5], (SPANS,), 0, 4) < 1).astype(jnp.int32), jax.random.fold_in(part_splits[5], 1), 0, 1),
        "new_slot": draw_new_slot(jax.random.fold_in(jax.random.fold_in(seeds[11], part), 71), part),
        "out_proj": noise(seeds[7], (D, D), D ** -0.5, 0.15625, ((0, 2),)),
        "ln_gain": jnp.clip(1.0 + 0.1 * jax.random.normal(seeds[8], (D,), jnp.float32), 0.5, 1.5),
        "ln_bias": draw_ln_bias(jax.random.fold_in(seeds[11], 71), part),
        "query_proj": draw_query_proj(jax.random.fold_in(seeds[11], 71), part),
    }


def reference(hidden, token_qkv, self_cache, cross_kv, cache_len, finished, new_slot, out_proj, ln_gain, ln_bias, query_proj):
    head_count = D // HEAD_DIM
    factor = HEAD_DIM ** (-0.5)
    new_query = token_qkv[0].astype(jnp.float32).reshape(SPANS, head_count, HEAD_DIM)
    new_key = token_qkv[1].astype(jnp.float32).reshape(SPANS, head_count, HEAD_DIM)
    new_value = token_qkv[2].astype(jnp.float32).reshape(SPANS, head_count, HEAD_DIM)
    cache_keys = self_cache[0].astype(jnp.float32).reshape(SPANS, SLOTS, head_count, HEAD_DIM)
    cache_values = self_cache[1].astype(jnp.float32).reshape(SPANS, SLOTS, head_count, HEAD_DIM)
    scores = jnp.einsum('chd,cthd->cht', new_query, cache_keys) * factor
    position = jnp.arange(SLOTS, dtype=jnp.int32)
    usable = position[None, None, :] < cache_len[:, None, None]
    scores = jnp.where(usable, scores, -1e+30)
    own_score = lax.optimization_barrier(jnp.sum(new_query * new_key, axis=-1)) * factor
    highest = jnp.maximum(lax.optimization_barrier(jnp.max(scores, axis=-1)), own_score)
    cache_weight = jnp.where(usable, jnp.exp(scores - highest[..., None]), 0.0)
    own_weight = jnp.exp(own_score - highest)
    total = lax.optimization_barrier(jnp.sum(cache_weight, axis=-1)) + own_weight
    cache_weight = (cache_weight / total[..., None]).astype(jnp.bfloat16)
    own_weight = (own_weight / total).astype(jnp.bfloat16)
    context = jnp.einsum('cht,cthd->chd', cache_weight.astype(jnp.float32), cache_values)
    context = context + own_weight.astype(jnp.float32)[..., None] * new_value
    context = context.astype(jnp.bfloat16).reshape(SPANS, D)
    resid = hidden.astype(jnp.float32) + jnp.dot(context, out_proj, preferred_element_type=jnp.float32)
    centre = lax.optimization_barrier(jnp.mean(resid, axis=-1, keepdims=True))
    spread = lax.optimization_barrier(jnp.mean((resid - centre) ** 2, axis=-1, keepdims=True))
    normed = ((resid - centre) * lax.rsqrt(spread + 1e-05) * ln_gain + ln_bias).astype(jnp.bfloat16)
    cross_query = jnp.dot(normed, query_proj, preferred_element_type=jnp.float32).astype(jnp.bfloat16)
    cross_query = cross_query.astype(jnp.float32).reshape(SPANS, head_count, HEAD_DIM)
    cross_keys = cross_kv[0].astype(jnp.float32).reshape(SPANS, ENC, head_count, HEAD_DIM)
    cross_values = cross_kv[1].astype(jnp.float32).reshape(SPANS, ENC, head_count, HEAD_DIM)
    cross_scores = jnp.einsum('chd,cthd->cht', cross_query, cross_keys) * factor
    cross_high = lax.optimization_barrier(jnp.max(cross_scores, axis=-1, keepdims=True))
    cross_exp = jnp.exp(cross_scores - cross_high)
    cross_weight = (cross_exp / lax.optimization_barrier(jnp.sum(cross_exp, axis=-1, keepdims=True))).astype(jnp.bfloat16)
    cross_context = jnp.einsum('cht,cthd->chd', cross_weight.astype(jnp.float32), cross_values).reshape(SPANS, D)
    alive = finished == 0
    decoded = jnp.where(alive[:, None], cross_context, 0.0).astype(jnp.bfloat16)
    slot_pos = position[None, :, None]
    length = cache_len[:, None, None]

    def extend(older, fresh):
        grown = jnp.where(slot_pos < length, older, jnp.where(slot_pos == length, fresh[:, None, :], jnp.zeros_like(older)))
        return jnp.where(alive[:, None, None], grown, jnp.zeros_like(older))
    updated = jnp.stack([extend(self_cache[0], token_qkv[1]), extend(self_cache[1], token_qkv[2])])
    moved_cache = jnp.zeros_like(self_cache).at[:, new_slot].set(updated)
    moved_out = jnp.zeros((SPANS, D), jnp.bfloat16).at[new_slot].set(decoded)
    return (moved_cache, moved_out)
```

```python
import functools

import jax
import jax.numpy as jnp
from jax import lax
from jax.experimental import pallas as pl
from jax.experimental.pallas import tpu as pltpu
from jax.sharding import PartitionSpec as P

HEAD_DIM = 64
REACH = 3
MESH = pl.DeviceIdType.MESH
DISTANCES = [3, -3, 2, -2, 1, -1]


def attend(query, keys, values, length, own):
    slots, width = keys.shape
    heads = width // HEAD_DIM
    rows = -(-heads // 16) * 16
    row = lax.broadcasted_iota(jnp.int32, (rows, width), 0)
    column = lax.broadcasted_iota(jnp.int32, (rows, width), 1)
    low = row * HEAD_DIM
    mine = (column >= low) & (column < low + HEAD_DIM)
    spread = jnp.where(mine, query.astype(jnp.float32), 0.0)
    factor = HEAD_DIM ** (-0.5)
    scores = (
        lax.dot_general(
            spread.astype(jnp.bfloat16),
            keys,
            (((1,), (1,)), ((), ())),
            preferred_element_type=jnp.float32,
        )
        * factor
    )
    if length is not None:
        usable = lax.broadcasted_iota(jnp.int32, (rows, slots), 1) < length
        scores = jnp.where(usable, scores, -1e30)
    highest = jnp.max(scores, axis=-1, keepdims=True)
    if own is not None:
        new_key, new_value = own
        own_score = jnp.sum(spread * new_key.astype(jnp.float32), axis=-1, keepdims=True) * factor
        highest = jnp.maximum(highest, own_score)
    weight = jnp.exp(scores - highest)
    if length is not None:
        weight = jnp.where(usable, weight, 0.0)
    total = jnp.sum(weight, axis=-1, keepdims=True)
    if own is not None:
        own_weight = jnp.exp(own_score - highest)
        total = total + own_weight
    weight = (weight / total).astype(jnp.bfloat16)
    mixed = jnp.dot(weight, values, preferred_element_type=jnp.float32)
    if own is not None:
        own_weight = (own_weight / total).astype(jnp.bfloat16).astype(jnp.float32)
        mixed = mixed + own_weight * new_value.astype(jnp.float32)
    return jnp.sum(jnp.where(mine, mixed, 0.0), axis=0, keepdims=True)


def kernel(
    count,
    cores,
    cache_len,
    finished,
    new_slot,
    hidden,
    token_qkv,
    self_cache,
    ln_gain,
    ln_bias,
    cross_hbm,
    out_proj_hbm,
    query_proj_hbm,
    moved_cache,
    moved_out,
    cross,
    out_proj,
    query_proj,
    updated,
    parcel,
    arrived,
    mark,
    mark_in,
    line,
    line_in,
    part,
    part_in,
    load_sem,
    cache_sems,
    mark_sems,
    line_sems,
    part_sems,
):
    spans, width = hidden.shape
    slots, local = self_cache.shape[2:]
    me = lax.axis_index("batch")
    core = lax.axis_index("mp")
    loads = [
        pltpu.make_async_copy(source, target, load_sem.at[i])
        for i, (source, target) in enumerate(
            [(out_proj_hbm, out_proj), (query_proj_hbm, query_proj), (cross_hbm, cross)]
        )
    ]
    for load in loads:
        load.start()

    barrier = pltpu.get_barrier_semaphore()
    targets = [lax.rem(me + distance + count, count) for distance in DISTANCES]
    for target in targets:
        pl.semaphore_signal(barrier, inc=1, device_id={"batch": target}, device_id_type=MESH)
    others = [lax.rem(core + k, cores) for k in range(1, cores)]
    for other in others:
        pl.semaphore_signal(barrier, inc=1, device_id={"mp": other}, device_id_type=MESH)

    half = count // 2
    alive, offset, place = [], [], []
    for c in range(spans):
        slot = new_slot[c]
        owner = lax.div(slot, spans)
        offset.append(lax.rem(owner - me + half + count, count) - half)
        place.append(lax.rem(slot, spans))
        alive.append(jnp.where(finished[c] == 0, 1, 0))

    position = lax.broadcasted_iota(jnp.int32, (slots, local), 0)
    for c in range(spans):
        length = cache_len[c]
        older = jnp.where(position < length * alive[c], 1.0, 0.0).astype(jnp.bfloat16)
        fresh = jnp.where(position == jnp.where(alive[c] == 1, length, -1), 1.0, 0.0).astype(
            jnp.bfloat16
        )
        for a in range(2):
            updated[a, c] = self_cache[a, c] * older + token_qkv[1 + a, c : c + 1, :] * fresh

    def flag(value, shape):
        return jnp.full(shape, jnp.where(value, 1.0, 0.0), jnp.float32).astype(jnp.bfloat16)

    marker_row = lax.broadcasted_iota(jnp.int32, mark.shape[1:], 0)
    for i, distance in enumerate(DISTANCES):
        marker = jnp.zeros(mark.shape[1:], jnp.float32)
        for c in range(spans):
            at = jnp.where(offset[c] == distance, place[c], -1)
            marker = jnp.where(marker_row == at, 1.0, marker)
        mark[i] = marker.astype(jnp.bfloat16)

    def send(source, target, sems, i, distance):
        return pltpu.make_async_remote_copy(
            src_ref=source,
            dst_ref=target,
            send_sem=sems.at[0, i],
            recv_sem=sems.at[1, i],
            device_id={"batch": targets[i]},
            device_id_type=MESH,
        )

    pl.semaphore_wait(barrier, len(targets) + len(others))
    mark_copies, cache_copies = [], []
    for i, distance in enumerate(DISTANCES):
        copy = send(mark.at[i], mark_in.at[i], mark_sems, i, distance)
        copy.start()
        mark_copies.append(copy)
    for i, distance in enumerate(DISTANCES):
        for a in range(2):
            total = updated[a, 0] * flag(offset[0] == distance, (1, local))
            for c in range(1, spans):
                total = total + updated[a, c] * flag(offset[c] == distance, (1, local))
            parcel[i, a] = total
        copy = send(parcel.at[i], arrived.at[i], cache_sems, i, distance)
        copy.start()
        cache_copies.append(copy)

    for l in range(spans):
        for a in range(2):
            total = updated[a, 0] * flag((offset[0] == 0) & (place[0] == l), (1, local))
            for c in range(1, spans):
                keep = flag((offset[c] == 0) & (place[c] == l), (1, local))
                total = total + updated[a, c] * keep
            moved_cache[a, l] = total

    contexts = []
    for c in range(spans):
        query, key, value = (token_qkv[k, c : c + 1, :] for k in range(3))
        contexts.append(
            attend(query, self_cache[0, c], self_cache[1, c], cache_len[c], (key, value))
        )
    pad = part.shape[0] - spans
    context = jnp.concatenate(contexts + [jnp.zeros((pad, local), jnp.float32)], 0)
    context = context.astype(jnp.bfloat16)
    loads[0].wait()
    part[...] = jnp.dot(context, out_proj[...], preferred_element_type=jnp.float32)
    part_copies = []
    for k, other in enumerate(others):
        copy = pltpu.make_async_remote_copy(
            src_ref=part,
            dst_ref=part_in.at[k],
            send_sem=part_sems.at[0, k],
            recv_sem=part_sems.at[1, k],
            device_id={"mp": other},
            device_id_type=MESH,
        )
        copy.start()
        part_copies.append(copy)
    loads[1].wait()
    loads[2].wait()
    for copy in part_copies:
        copy.wait()
    summed = part[...]
    for k in range(len(others)):
        summed = summed + part_in[k]
    resid = hidden[...].astype(jnp.float32) + summed[:spans]
    centre = jnp.mean(resid, axis=-1, keepdims=True)
    spread = jnp.mean((resid - centre) ** 2, axis=-1, keepdims=True)
    gain = ln_gain[...].reshape(1, width)
    bias = ln_bias[...].reshape(1, width)
    normed = (resid - centre) * lax.rsqrt(spread + 1e-05) * gain + bias
    normed = jnp.concatenate([normed, jnp.zeros((pad, width), jnp.float32)], 0)
    query = jnp.dot(
        normed.astype(jnp.bfloat16), query_proj[...], preferred_element_type=jnp.float32
    ).astype(jnp.bfloat16).astype(jnp.float32)
    decoded = []
    for c in range(spans):
        mixed = attend(query[c : c + 1], cross[0, c], cross[1, c], None, None)
        decoded.append(mixed * jnp.where(alive[c] == 1, 1.0, 0.0))

    line_copies = []
    blank = jnp.zeros((line.shape[1] - 1, local), jnp.float32)
    for i, distance in enumerate(DISTANCES):
        row = jnp.zeros((1, local), jnp.float32)
        for c in range(spans):
            row = row + decoded[c] * jnp.where(offset[c] == distance, 1.0, 0.0)
        line[i] = jnp.concatenate([row, blank], 0).astype(jnp.bfloat16)
        copy = send(line.at[i], line_in.at[i], line_sems, i, distance)
        copy.start()
        line_copies.append(copy)

    rows = []
    for l in range(spans):
        row = jnp.zeros((1, local), jnp.float32)
        for c in range(spans):
            keep = (offset[c] == 0) & (place[c] == l)
            row = row + decoded[c] * jnp.where(keep, 1.0, 0.0)
        rows.append(row)
    for i in range(len(DISTANCES)):
        mark_copies[i].wait()
        cache_copies[i].wait()
        for l in range(spans):
            taken = mark_in[i, l : l + 1, :]
            for a in range(2):
                moved_cache[a, l] = moved_cache[a, l] + arrived[i, a] * taken
    for i in range(len(DISTANCES)):
        line_copies[i].wait()
        for l in range(spans):
            taken = mark_in[i, l : l + 1, :].astype(jnp.float32)
            rows[l] = rows[l] + line_in[i, 0:1, :].astype(jnp.float32) * taken
    moved_out[...] = jnp.concatenate(rows, 0).astype(jnp.bfloat16)


def body(
    hidden,
    token_qkv,
    self_cache,
    cross_kv,
    cache_len,
    finished,
    new_slot,
    out_proj,
    ln_gain,
    ln_bias,
    query_proj,
):
    count, cores = lax.axis_size("batch"), lax.axis_size("mp")
    spans, width = hidden.shape
    slots, local = self_cache.shape[2:]
    moves = len(DISTANCES)
    smem = pl.BlockSpec(memory_space=pltpu.SMEM)
    vmem = pl.BlockSpec(memory_space=pltpu.VMEM)
    away = pl.BlockSpec(memory_space=pl.ANY)
    bf16, f32 = jnp.bfloat16, jnp.float32
    return pl.pallas_call(
        functools.partial(kernel, count, cores),
        out_shape=(
            jax.ShapeDtypeStruct(self_cache.shape, bf16),
            jax.ShapeDtypeStruct((spans, local), bf16),
        ),
        in_specs=[smem] * 3 + [vmem] * 5 + [away] * 3,
        out_specs=(vmem, vmem),
        scratch_shapes=[
            pltpu.VMEM(cross_kv.shape, bf16),
            pltpu.VMEM(out_proj.shape, bf16),
            pltpu.VMEM(query_proj.shape, bf16),
            pltpu.VMEM(self_cache.shape, bf16),
            pltpu.VMEM((moves, 2, slots, local), bf16),
            pltpu.VMEM((moves, 2, slots, local), bf16),
            pltpu.VMEM((moves, 16, local), bf16),
            pltpu.VMEM((moves, 16, local), bf16),
            pltpu.VMEM((moves, 16, local), bf16),
            pltpu.VMEM((moves, 16, local), bf16),
            pltpu.VMEM((8, width), f32),
            pltpu.VMEM((cores - 1, 8, width), f32),
            pltpu.SemaphoreType.DMA((3,)),
            pltpu.SemaphoreType.DMA((2, moves)),
            pltpu.SemaphoreType.DMA((2, moves)),
            pltpu.SemaphoreType.DMA((2, moves)),
            pltpu.SemaphoreType.DMA((2, cores - 1)),
        ],
        compiler_params=pltpu.CompilerParams(collective_id=0, has_side_effects=True),
    )(
        cache_len,
        finished,
        new_slot,
        hidden,
        token_qkv,
        self_cache,
        ln_gain,
        ln_bias,
        cross_kv,
        out_proj,
        query_proj,
    )


def solution(mesh):
    placed = (
        P(("groups", "batch"), None),
        P(None, ("groups", "batch"), "mp"),
        P(None, ("groups", "batch"), None, "mp"),
        P(None, ("groups", "batch"), None, "mp"),
        P(("groups", "batch")),
        P(("groups", "batch")),
        P(("groups", "batch")),
        P("mp", None),
        P(),
        P(),
        P(None, "mp"),
    )
    return jax.shard_map(
        body,
        mesh=mesh,
        in_specs=placed,
        out_specs=(P(None, ("groups", "batch"), None, "mp"), P(("groups", "batch"), "mp")),
        check_vma=False,
    )
```

```python
import functools

import jax
import jax.numpy as jnp
from jax import lax
from jax.experimental import pallas as pl
from jax.experimental.pallas import tpu as pltpu
from jax.sharding import PartitionSpec as P

HEAD_DIM = 64
REACH = 3
MESH = pl.DeviceIdType.MESH
DISTANCES = [3, -3, 2, -2, 1, -1]
ROWS = 16
LAG = 3
EARLY = 1


def attend(query, keys, values, length, own):
    slots, width = keys.shape
    heads = width // HEAD_DIM
    rows = -(-heads // 16) * 16
    row = lax.broadcasted_iota(jnp.int32, (rows, width), 0)
    column = lax.broadcasted_iota(jnp.int32, (rows, width), 1)
    low = row * HEAD_DIM
    mine = (column >= low) & (column < low + HEAD_DIM)
    spread = jnp.where(mine, query.astype(jnp.float32), 0.0)
    factor = HEAD_DIM ** (-0.5)
    scores = (
        lax.dot_general(
            spread.astype(jnp.bfloat16),
            keys,
            (((1,), (1,)), ((), ())),
            preferred_element_type=jnp.float32,
        )
        * factor
    )
    if length is not None:
        usable = lax.broadcasted_iota(jnp.int32, (rows, slots), 1) < length
        scores = jnp.where(usable, scores, -1e30)
    highest = jnp.max(scores, axis=-1, keepdims=True)
    if own is not None:
        new_key, new_value = own
        own_score = jnp.sum(spread * new_key.astype(jnp.float32), axis=-1, keepdims=True) * factor
        highest = jnp.maximum(highest, own_score)
    weight = jnp.exp(scores - highest)
    if length is not None:
        weight = jnp.where(usable, weight, 0.0)
    total = jnp.sum(weight, axis=-1, keepdims=True)
    if own is not None:
        own_weight = jnp.exp(own_score - highest)
        total = total + own_weight
    weight = (weight / total).astype(jnp.bfloat16)
    mixed = jnp.dot(weight, values, preferred_element_type=jnp.float32)
    if own is not None:
        own_weight = (own_weight / total).astype(jnp.bfloat16).astype(jnp.float32)
        mixed = mixed + own_weight * new_value.astype(jnp.float32)
    return jnp.sum(jnp.where(mine, mixed, 0.0), axis=0, keepdims=True)


def kernel(
    count,
    cores,
    cache_len,
    finished,
    new_slot,
    hidden,
    token_qkv,
    self_cache,
    ln_gain,
    ln_bias,
    cross_hbm,
    out_proj_hbm,
    query_proj_hbm,
    moved_cache,
    moved_out,
    cross,
    out_proj,
    query_proj,
    updated,
    parcel,
    arrived,
    mark,
    mark_in,
    line,
    line_in,
    part,
    part_in,
    load_sem,
    cache_sems,
    mark_sems,
    line_sems,
    part_sems,
):
    spans, width = hidden.shape
    slots, local = self_cache.shape[2:]
    me = lax.axis_index("batch")
    core = lax.axis_index("mp")
    loads = [
        pltpu.make_async_copy(source, target, load_sem.at[i])
        for i, (source, target) in enumerate(
            [(out_proj_hbm, out_proj), (query_proj_hbm, query_proj), (cross_hbm, cross)]
        )
    ]
    for load in loads:
        load.start()

    barrier = pltpu.get_barrier_semaphore()
    targets = [lax.rem(me + distance + count, count) for distance in DISTANCES]
    for target in targets:
        pl.semaphore_signal(barrier, inc=1, device_id={"batch": target}, device_id_type=MESH)
    others = [lax.rem(core + k, cores) for k in range(1, cores)]
    for other in others:
        pl.semaphore_signal(barrier, inc=1, device_id={"mp": other}, device_id_type=MESH)

    half = count // 2
    alive, offset, place = [], [], []
    for c in range(spans):
        slot = new_slot[c]
        owner = lax.div(slot, spans)
        offset.append(lax.rem(owner - me + half + count, count) - half)
        place.append(lax.rem(slot, spans))
        alive.append(jnp.where(finished[c] == 0, 1, 0))

    position = lax.broadcasted_iota(jnp.int32, (slots, local), 0)
    for c in range(spans):
        length = cache_len[c]
        older = jnp.where(position < length * alive[c], 1.0, 0.0).astype(jnp.bfloat16)
        fresh = jnp.where(position == jnp.where(alive[c] == 1, length, -1), 1.0, 0.0).astype(
            jnp.bfloat16
        )
        for a in range(2):
            updated[a, c] = self_cache[a, c] * older + token_qkv[1 + a, c : c + 1, :] * fresh

    def flag(value, shape):
        return jnp.full(shape, jnp.where(value, 1.0, 0.0), jnp.float32).astype(jnp.bfloat16)

    marker_row = lax.broadcasted_iota(jnp.int32, mark.shape[1:], 0)
    for i, distance in enumerate(DISTANCES):
        marker = jnp.zeros(mark.shape[1:], jnp.float32)
        for c in range(spans):
            at = jnp.where(offset[c] == distance, place[c], -1)
            marker = jnp.where(marker_row == at, 1.0, marker)
        mark[i] = marker.astype(jnp.bfloat16)

    def send(source, target, sems, i, distance):
        return pltpu.make_async_remote_copy(
            src_ref=source,
            dst_ref=target,
            send_sem=sems.at[0, i],
            recv_sem=sems.at[1, i],
            device_id={"batch": targets[i]},
            device_id_type=MESH,
        )

    pl.semaphore_wait(barrier, len(targets) + len(others))
    mark_copies, cache_copies = [], []
    for i, distance in enumerate(DISTANCES):
        copy = send(mark.at[i], mark_in.at[i], mark_sems, i, distance)
        copy.start()
        mark_copies.append(copy)
    for i, distance in enumerate(DISTANCES):
        for a in range(2):
            total = updated[a, 0] * flag(offset[0] == distance, (1, local))
            for c in range(1, spans):
                total = total + updated[a, c] * flag(offset[c] == distance, (1, local))
            parcel[i, a] = total
        copy = send(parcel.at[i], arrived.at[i], cache_sems, i, distance)
        copy.start()
        cache_copies.append(copy)

    for l in range(spans):
        for a in range(2):
            total = updated[a, 0] * flag((offset[0] == 0) & (place[0] == l), (1, local))
            for c in range(1, spans):
                keep = flag((offset[c] == 0) & (place[c] == l), (1, local))
                total = total + updated[a, c] * keep
            moved_cache[a, l] = total

    contexts = []
    for c in range(spans):
        query, key, value = (token_qkv[k, c : c + 1, :] for k in range(3))
        contexts.append(
            attend(query, self_cache[0, c], self_cache[1, c], cache_len[c], (key, value))
        )
    pad = part.shape[0] - spans
    context = jnp.concatenate(contexts + [jnp.zeros((pad, local), jnp.float32)], 0)
    context = context.astype(jnp.bfloat16)
    loads[0].wait()
    part[...] = jnp.dot(context, out_proj[...], preferred_element_type=jnp.float32)
    part_copies = []
    for k, other in enumerate(others):
        copy = pltpu.make_async_remote_copy(
            src_ref=part,
            dst_ref=part_in.at[k],
            send_sem=part_sems.at[0, k],
            recv_sem=part_sems.at[1, k],
            device_id={"mp": other},
            device_id_type=MESH,
        )
        copy.start()
        part_copies.append(copy)
    loads[1].wait()
    loads[2].wait()
    for copy in part_copies:
        copy.wait()
    summed = part[...]
    for k in range(len(others)):
        summed = summed + part_in[k]
    resid = hidden[...].astype(jnp.float32) + summed[:spans]
    centre = jnp.mean(resid, axis=-1, keepdims=True)
    spread = jnp.mean((resid - centre) ** 2, axis=-1, keepdims=True)
    gain = ln_gain[...].reshape(1, width)
    bias = ln_bias[...].reshape(1, width)
    normed = (resid - centre) * lax.rsqrt(spread + 1e-05) * gain + bias
    normed = jnp.concatenate([normed, jnp.zeros((pad, width), jnp.float32)], 0)
    query = jnp.dot(
        normed.astype(jnp.bfloat16), query_proj[...], preferred_element_type=jnp.float32
    ).astype(jnp.bfloat16).astype(jnp.float32)
    decoded = []
    for c in range(spans):
        mixed = attend(query[c : c + 1], cross[0, c], cross[1, c], None, None)
        decoded.append(mixed * jnp.where(alive[c] == 1, 1.0, 0.0))

    line_copies = []
    blank = jnp.zeros((line.shape[1] - 1, local), jnp.float32)
    for i, distance in enumerate(DISTANCES):
        row = jnp.zeros((1, local), jnp.float32)
        for c in range(spans):
            row = row + decoded[c] * jnp.where(offset[c] == distance, 1.0, 0.0)
        line[i] = jnp.concatenate([row, blank], 0).astype(jnp.bfloat16)
        copy = send(line.at[i], line_in.at[i], line_sems, i, distance)
        copy.start()
        line_copies.append(copy)

    rows = []
    for l in range(spans):
        row = jnp.zeros((1, local), jnp.float32)
        for c in range(spans):
            keep = (offset[c] == 0) & (place[c] == l)
            row = row + decoded[c] * jnp.where(keep, 1.0, 0.0)
        rows.append(row)
    for i in range(len(DISTANCES)):
        mark_copies[i].wait()
        cache_copies[i].wait()
        for l in range(spans):
            taken = mark_in[i, l : l + 1, :]
            for a in range(2):
                moved_cache[a, l] = moved_cache[a, l] + arrived[i, a] * taken
    for i in range(len(DISTANCES)):
        line_copies[i].wait()
        for l in range(spans):
            taken = mark_in[i, l : l + 1, :].astype(jnp.float32)
            rows[l] = rows[l] + line_in[i, 0:1, :].astype(jnp.float32) * taken
    moved_out[...] = jnp.concatenate(rows, 0).astype(jnp.bfloat16)


def relay_kernel(
    count,
    cores,
    cache_len,
    finished,
    new_slot,
    hidden,
    token_qkv,
    self_cache,
    ln_gain,
    ln_bias,
    cross_hbm,
    out_proj_hbm,
    query_proj_hbm,
    moved_cache,
    moved_out,
    cross,
    out_proj,
    query_proj,
    own,
    raw_in,
    cross_out,
    cross_in,
    kept,
    final_out,
    final_in,
    pick,
    label,
    label_in,
    mark,
    mark_in,
    line,
    line_in,
    part,
    part_in,
    load_sem,
    raw_send,
    raw_recv,
    hop_sems,
    label_send,
    label_recv,
    mark_sems,
    line_sems,
    part_sems,
):
    spans, width = hidden.shape
    slots, local = self_cache.shape[2:]
    steps, _, rows_per, _ = own.shape
    per = steps // 2
    me = lax.axis_index("batch")
    core = lax.axis_index("mp")
    level, column = lax.div(me, 2), lax.rem(me, 2)
    left = level < REACH - 1
    inner = (level == 1) | (level == REACH - 1)
    outer = jnp.logical_not(inner)
    loads = [
        pltpu.make_async_copy(source, target, load_sem.at[i])
        for i, (source, target) in enumerate(
            [(out_proj_hbm, out_proj), (query_proj_hbm, query_proj), (cross_hbm, cross)]
        )
    ]
    for load in loads:
        load.start()

    barrier = pltpu.get_barrier_semaphore()
    targets = [lax.rem(me + distance + count, count) for distance in DISTANCES]
    for target in targets:
        pl.semaphore_signal(barrier, inc=1, device_id={"batch": target}, device_id_type=MESH)
    others = [lax.rem(core + k, cores) for k in range(1, cores)]
    for other in others:
        pl.semaphore_signal(barrier, inc=1, device_id={"mp": other}, device_id_type=MESH)

    mate_level = jnp.where(level == 0, 1, jnp.where(level == 1, 0, jnp.where(level == 2, 3, 2)))
    mate = mate_level * 2 + column
    mate_aside = mate_level * 2 + 1 - column
    aside = level * 2 + 1 - column
    across = (REACH - level) * 2 + column
    beyond = (REACH - mate_level) * 2 + column

    half = count // 2
    alive, offset, place = [], [], []
    for c in range(spans):
        slot = new_slot[c]
        owner = lax.div(slot, spans)
        offset.append(lax.rem(owner - me + half + count, count) - half)
        place.append(lax.rem(slot, spans))
        alive.append(jnp.where(finished[c] == 0, 1, 0))

    def to(node, source, target, sent, received):
        return pltpu.make_async_remote_copy(
            src_ref=source,
            dst_ref=target,
            send_sem=sent,
            recv_sem=received,
            device_id={"batch": node},
            device_id_type=MESH,
        )

    def raw_copy(node, lane, way, k):
        return to(node, own.at[k], raw_in.at[way, k], raw_send.at[lane, k], raw_recv.at[way, k])

    def cross_copy(k):
        return to(across, cross_out.at[k], cross_in.at[k], hop_sems.at[0, k], hop_sems.at[1, k])

    def final_copy(k):
        return to(mate, final_out.at[k], final_in.at[k], hop_sems.at[2, k], hop_sems.at[3, k])

    def label_copy(node, lane, way):
        return to(node, label, label_in.at[way], label_send.at[lane], label_recv.at[way])

    def mark_copy(i):
        return to(targets[i], mark.at[i], mark_in.at[i], mark_sems.at[0, i], mark_sems.at[1, i])

    def line_copy(i):
        return to(targets[i], line.at[i], line_in.at[i], line_sems.at[0, i], line_sems.at[1, i])

    label_row = lax.broadcasted_iota(jnp.int32, label.shape, 0)
    labels = jnp.zeros(label.shape, jnp.int32)
    for c in range(spans):
        labels = jnp.where(label_row == c, new_slot[c], labels)
    label[...] = labels.astype(jnp.float32)
    marker_row = lax.broadcasted_iota(jnp.int32, mark.shape[1:], 0)
    for i, distance in enumerate(DISTANCES):
        marker = jnp.zeros(mark.shape[1:], jnp.float32)
        for c in range(spans):
            at = jnp.where(offset[c] == distance, place[c], -1)
            marker = jnp.where(marker_row == at, 1.0, marker)
        mark[i] = marker.astype(jnp.bfloat16)

    pl.semaphore_wait(barrier, len(targets) + len(others))

    position = lax.broadcasted_iota(jnp.int32, (rows_per, local), 0)
    ends = [cache_len[c] * alive[c] for c in range(spans)]
    fresh_at = [jnp.where(alive[c] == 1, cache_len[c], -1) for c in range(spans)]

    def grow(k, _):
        a, r = lax.div(k, per), lax.rem(k, per)
        start = pl.multiple_of(r * rows_per, rows_per)
        at = position + start
        for c in range(spans):
            older = jnp.where(at < ends[c], 1.0, 0.0).astype(jnp.bfloat16)
            fresh = jnp.where(at == fresh_at[c], 1.0, 0.0).astype(jnp.bfloat16)
            new = jnp.where(a == 0, token_qkv[1, c : c + 1, :].astype(jnp.float32),
                            token_qkv[2, c : c + 1, :].astype(jnp.float32)).astype(jnp.bfloat16)
            own[k, c] = self_cache[a, c, pl.ds(start, rows_per), :] * older + new * fresh

        @pl.when(outer)
        def _():
            raw_copy(mate, 0, 0, k).start()
            raw_copy(mate_aside, 1, 1, k).start()

        @pl.when(inner)
        def _():
            raw_copy(aside, 0, 2, k).start()

        return 0

    @pl.when(outer)
    def _():
        label_copy(mate, 0, 0).start()
        label_copy(mate_aside, 1, 1).start()

    @pl.when(inner)
    def _():
        label_copy(aside, 0, 2).start()

    lax.fori_loop(0, steps, grow, 0)
    for i in range(len(DISTANCES)):
        mark_copy(i).start()

    def self_part():
        contexts = []
        for c in range(spans):
            query, key, value = (token_qkv[k, c : c + 1, :] for k in range(3))
            contexts.append(
                attend(query, self_cache[0, c], self_cache[1, c], cache_len[c], (key, value))
            )
        context = jnp.concatenate(contexts + [jnp.zeros((pad, local), jnp.float32)], 0)
        context = context.astype(jnp.bfloat16)
        loads[0].wait()
        part[...] = jnp.dot(context, out_proj[...], preferred_element_type=jnp.float32)

    def part_copy(k):
        return pltpu.make_async_remote_copy(
            src_ref=part,
            dst_ref=part_in.at[k],
            send_sem=part_sems.at[0, k],
            recv_sem=part_sems.at[1, k],
            device_id={"mp": others[k]},
            device_id_type=MESH,
        )

    pad = part.shape[0] - spans
    self_part()
    for k in range(len(others)):
        part_copy(k).start()

    @pl.when(inner)
    def _():
        for way in range(3):
            label_copy(mate, 0, way).wait_recv()
        sources = [label] + [label_in.at[way] for way in range(3)]
        nodes = [me, mate, across, beyond]
        for s, source in enumerate(sources):
            for c in range(spans):
                held = jnp.broadcast_to(source[c : c + 1, :], (rows_per, local))
                for d, node in enumerate(nodes):
                    for l in range(spans):
                        wanted = jnp.full((rows_per, local), node * spans + l, jnp.int32)
                        pick[s * spans + c, d * spans + l] = jnp.where(
                            held == wanted.astype(jnp.float32), 1.0, 0.0
                        ).astype(jnp.bfloat16)

    def merge(k, _):
        for way in range(3):
            raw_copy(mate, 0, way, k).wait_recv()
        blocks = [own[k, c] for c in range(spans)]
        for way in range(3):
            blocks += [raw_in[way, k, c] for c in range(spans)]

        def gathered(d):
            total = blocks[0] * pick[0, d]
            for s in range(1, len(blocks)):
                total = total + blocks[s] * pick[s, d]
            return total

        for d in range(2 * spans):
            cross_out[k, d] = gathered(2 * spans + d)
        cross_copy(k).start()
        for d in range(2 * spans):
            kept[k, d] = gathered(d)
        return 0

    def finish(k, _):
        cross_copy(k).wait_recv()
        a, r = lax.div(k, per), lax.rem(k, per)
        start = pl.multiple_of(r * rows_per, rows_per)
        for l in range(spans):
            final_out[k, l] = kept[k, spans + l] + cross_in[k, spans + l]
        final_copy(k).start()
        for l in range(spans):
            moved_cache[a, l, pl.ds(start, rows_per), :] = kept[k, l] + cross_in[k, l]
        return 0

    def both(k, _):
        merge(k, 0)
        finish(k - LAG, 0)
        return 0

    @pl.when(inner)
    def _():
        lax.fori_loop(0, EARLY, merge, 0)

    loads[1].wait()
    loads[2].wait()
    for k in range(len(others)):
        part_copy(k).wait()
    summed = part[...]
    for k in range(len(others)):
        summed = summed + part_in[k]
    resid = hidden[...].astype(jnp.float32) + summed[:spans]
    centre = jnp.mean(resid, axis=-1, keepdims=True)
    spread = jnp.mean((resid - centre) ** 2, axis=-1, keepdims=True)
    gain = ln_gain[...].reshape(1, width)
    bias = ln_bias[...].reshape(1, width)
    normed = (resid - centre) * lax.rsqrt(spread + 1e-05) * gain + bias
    normed = jnp.concatenate([normed, jnp.zeros((pad, width), jnp.float32)], 0)
    query = jnp.dot(
        normed.astype(jnp.bfloat16), query_proj[...], preferred_element_type=jnp.float32
    ).astype(jnp.bfloat16).astype(jnp.float32)

    @pl.when(inner)
    def _():
        lax.fori_loop(EARLY, LAG, merge, 0)

    decoded = []
    for c in range(spans):
        mixed = attend(query[c : c + 1], cross[0, c], cross[1, c], None, None)
        decoded.append(mixed * jnp.where(alive[c] == 1, 1.0, 0.0))

    blank = jnp.zeros((line.shape[1] - 1, local), jnp.float32)
    for i, distance in enumerate(DISTANCES):
        row = jnp.zeros((1, local), jnp.float32)
        for c in range(spans):
            row = row + decoded[c] * jnp.where(offset[c] == distance, 1.0, 0.0)
        line[i] = jnp.concatenate([row, blank], 0).astype(jnp.bfloat16)
        line_copy(i).start()

    @pl.when(inner)
    def _():
        lax.fori_loop(LAG, steps, both, 0)

    rows = []
    for l in range(spans):
        row = jnp.zeros((1, local), jnp.float32)
        for c in range(spans):
            keep = (offset[c] == 0) & (place[c] == l)
            row = row + decoded[c] * jnp.where(keep, 1.0, 0.0)
        rows.append(row)
    for i in range(len(DISTANCES)):
        mark_copy(i).wait()
        line_copy(i).wait()
        for l in range(spans):
            taken = mark_in[i, l : l + 1, :].astype(jnp.float32)
            rows[l] = rows[l] + line_in[i, 0:1, :].astype(jnp.float32) * taken
    moved_out[...] = jnp.concatenate(rows, 0).astype(jnp.bfloat16)

    def land(k, _):
        final_copy(k).wait_recv()
        a, r = lax.div(k, per), lax.rem(k, per)
        start = pl.multiple_of(r * rows_per, rows_per)
        for l in range(spans):
            moved_cache[a, l, pl.ds(start, rows_per), :] = final_in[k, l]
        return 0

    def outer_sent(k, _):
        raw_copy(mate, 0, 0, k).wait_send()
        raw_copy(mate_aside, 1, 1, k).wait_send()
        return 0

    def inner_sent(k, _):
        raw_copy(aside, 0, 2, k).wait_send()
        cross_copy(k).wait_send()
        final_copy(k).wait_send()
        return 0

    @pl.when(inner)
    def _():
        lax.fori_loop(steps - LAG, steps, finish, 0)
        label_copy(aside, 0, 2).wait_send()
        lax.fori_loop(0, steps, inner_sent, 0)

    @pl.when(outer)
    def _():
        lax.fori_loop(0, steps, land, 0)
        label_copy(mate, 0, 0).wait_send()
        label_copy(mate_aside, 1, 1).wait_send()
        lax.fori_loop(0, steps, outer_sent, 0)


def body(
    hidden,
    token_qkv,
    self_cache,
    cross_kv,
    cache_len,
    finished,
    new_slot,
    out_proj,
    ln_gain,
    ln_bias,
    query_proj,
):
    count, cores = lax.axis_size("batch"), lax.axis_size("mp")
    spans, width = hidden.shape
    slots, local = self_cache.shape[2:]
    moves = len(DISTANCES)
    smem = pl.BlockSpec(memory_space=pltpu.SMEM)
    vmem = pl.BlockSpec(memory_space=pltpu.VMEM)
    away = pl.BlockSpec(memory_space=pl.ANY)
    bf16, f32 = jnp.bfloat16, jnp.float32
    operands = (
        cache_len,
        finished,
        new_slot,
        hidden,
        token_qkv,
        self_cache,
        ln_gain,
        ln_bias,
        cross_kv,
        out_proj,
        query_proj,
    )
    parcels = pltpu.VMEM((moves, 2, slots, local), bf16)
    tiles = pltpu.VMEM((moves, 16, local), bf16)
    dma = pltpu.SemaphoreType.DMA
    inputs = [pltpu.VMEM(array.shape, bf16) for array in (cross_kv, out_proj, query_proj)]
    parts = [pltpu.VMEM((8, width), f32), pltpu.VMEM((cores - 1, 8, width), f32)]
    steps = 2 * slots // ROWS
    if count == 2 * (REACH + 1):
        function = relay_kernel

        def blocks(*lead):
            return pltpu.VMEM(lead + (ROWS, local), bf16)

        scratch = inputs + [
            blocks(steps, spans),
            blocks(3, steps, spans),
            blocks(steps, 2 * spans),
            blocks(steps, 2 * spans),
            blocks(steps, 2 * spans),
            blocks(steps, spans),
            blocks(steps, spans),
            blocks(4 * spans, 4 * spans),
            pltpu.VMEM((8, local), f32),
            pltpu.VMEM((3, 8, local), f32),
            tiles,
            tiles,
            tiles,
            tiles,
            *parts,
            dma((3,)),
            dma((2, steps)),
            dma((3, steps)),
            dma((4, steps)),
            dma((2,)),
            dma((3,)),
            dma((2, moves)),
            dma((2, moves)),
            dma((2, cores - 1)),
        ]
    else:
        function = kernel
        scratch = inputs + [
            pltpu.VMEM(self_cache.shape, bf16),
            parcels,
            parcels,
            tiles,
            tiles,
            tiles,
            tiles,
            *parts,
            dma((3,)),
            dma((2, moves)),
            dma((2, moves)),
            dma((2, moves)),
            dma((2, cores - 1)),
        ]
    return pl.pallas_call(
        functools.partial(function, count, cores),
        out_shape=(
            jax.ShapeDtypeStruct(self_cache.shape, bf16),
            jax.ShapeDtypeStruct((spans, local), bf16),
        ),
        in_specs=[smem] * 3 + [vmem] * 5 + [away] * 3,
        out_specs=(vmem, vmem),
        scratch_shapes=scratch,
        compiler_params=pltpu.CompilerParams(collective_id=0, has_side_effects=True),
    )(*operands)


def solution(mesh):
    placed = (
        P(("groups", "batch"), None),
        P(None, ("groups", "batch"), "mp"),
        P(None, ("groups", "batch"), None, "mp"),
        P(None, ("groups", "batch"), None, "mp"),
        P(("groups", "batch")),
        P(("groups", "batch")),
        P(("groups", "batch")),
        P("mp", None),
        P(),
        P(),
        P(None, "mp"),
    )
    return jax.shard_map(
        body,
        mesh=mesh,
        in_specs=placed,
        out_specs=(P(None, ("groups", "batch"), None, "mp"), P(("groups", "batch"), "mp")),
        check_vma=False,
    )
```

```python
import functools

import jax
import jax.numpy as jnp
from jax import lax
from jax.experimental import pallas as pl
from jax.experimental.pallas import tpu as pltpu
from jax.sharding import PartitionSpec as P

HEAD_DIM = 64
REACH = 3
MESH = pl.DeviceIdType.MESH
DISTANCES = [3, -3, 2, -2, 1, -1]
ROWS = 16
LAG = 3
EARLY = 1


def attend(query, keys, values, length, own):
    slots, width = keys.shape
    heads = width // HEAD_DIM
    rows = -(-heads // 16) * 16
    row = lax.broadcasted_iota(jnp.int32, (rows, width), 0)
    column = lax.broadcasted_iota(jnp.int32, (rows, width), 1)
    low = row * HEAD_DIM
    mine = (column >= low) & (column < low + HEAD_DIM)
    spread = jnp.where(mine, query.astype(jnp.float32), 0.0)
    factor = HEAD_DIM ** (-0.5)
    scores = (
        lax.dot_general(
            spread.astype(jnp.bfloat16),
            keys,
            (((1,), (1,)), ((), ())),
            preferred_element_type=jnp.float32,
        )
        * factor
    )
    if length is not None:
        usable = lax.broadcasted_iota(jnp.int32, (rows, slots), 1) < length
        scores = jnp.where(usable, scores, -1e30)
    highest = jnp.max(scores, axis=-1, keepdims=True)
    if own is not None:
        new_key, new_value = own
        own_score = jnp.sum(spread * new_key.astype(jnp.float32), axis=-1, keepdims=True) * factor
        highest = jnp.maximum(highest, own_score)
    weight = jnp.exp(scores - highest)
    if length is not None:
        weight = jnp.where(usable, weight, 0.0)
    total = jnp.sum(weight, axis=-1, keepdims=True)
    if own is not None:
        own_weight = jnp.exp(own_score - highest)
        total = total + own_weight
    weight = (weight / total).astype(jnp.bfloat16)
    mixed = jnp.dot(weight, values, preferred_element_type=jnp.float32)
    if own is not None:
        own_weight = (own_weight / total).astype(jnp.bfloat16).astype(jnp.float32)
        mixed = mixed + own_weight * new_value.astype(jnp.float32)
    return jnp.sum(jnp.where(mine, mixed, 0.0), axis=0, keepdims=True)


def kernel(
    count,
    cores,
    cache_len,
    finished,
    new_slot,
    hidden,
    token_qkv,
    self_cache,
    ln_gain,
    ln_bias,
    cross_hbm,
    out_proj_hbm,
    query_proj_hbm,
    moved_cache,
    moved_out,
    cross,
    out_proj,
    query_proj,
    updated,
    parcel,
    arrived,
    mark,
    mark_in,
    line,
    line_in,
    part,
    part_in,
    load_sem,
    cache_sems,
    mark_sems,
    line_sems,
    part_sems,
):
    spans, width = hidden.shape
    slots, local = self_cache.shape[2:]
    me = lax.axis_index("batch")
    core = lax.axis_index("mp")
    loads = [
        pltpu.make_async_copy(source, target, load_sem.at[i])
        for i, (source, target) in enumerate(
            [(out_proj_hbm, out_proj), (query_proj_hbm, query_proj), (cross_hbm, cross)]
        )
    ]
    for load in loads:
        load.start()

    barrier = pltpu.get_barrier_semaphore()
    targets = [lax.rem(me + distance + count, count) for distance in DISTANCES]
    for target in targets:
        pl.semaphore_signal(barrier, inc=1, device_id={"batch": target}, device_id_type=MESH)
    others = [lax.rem(core + k, cores) for k in range(1, cores)]
    for other in others:
        pl.semaphore_signal(barrier, inc=1, device_id={"mp": other}, device_id_type=MESH)

    half = count // 2
    alive, offset, place = [], [], []
    for c in range(spans):
        slot = new_slot[c]
        owner = lax.div(slot, spans)
        offset.append(lax.rem(owner - me + half + count, count) - half)
        place.append(lax.rem(slot, spans))
        alive.append(jnp.where(finished[c] == 0, 1, 0))

    position = lax.broadcasted_iota(jnp.int32, (slots, local), 0)
    for c in range(spans):
        length = cache_len[c]
        older = jnp.where(position < length * alive[c], 1.0, 0.0).astype(jnp.bfloat16)
        fresh = jnp.where(position == jnp.where(alive[c] == 1, length, -1), 1.0, 0.0).astype(
            jnp.bfloat16
        )
        for a in range(2):
            updated[a, c] = self_cache[a, c] * older + token_qkv[1 + a, c : c + 1, :] * fresh

    def flag(value, shape):
        return jnp.full(shape, jnp.where(value, 1.0, 0.0), jnp.float32).astype(jnp.bfloat16)

    marker_row = lax.broadcasted_iota(jnp.int32, mark.shape[1:], 0)
    for i, distance in enumerate(DISTANCES):
        marker = jnp.zeros(mark.shape[1:], jnp.float32)
        for c in range(spans):
            at = jnp.where(offset[c] == distance, place[c], -1)
            marker = jnp.where(marker_row == at, 1.0, marker)
        mark[i] = marker.astype(jnp.bfloat16)

    def send(source, target, sems, i, distance):
        return pltpu.make_async_remote_copy(
            src_ref=source,
            dst_ref=target,
            send_sem=sems.at[0, i],
            recv_sem=sems.at[1, i],
            device_id={"batch": targets[i]},
            device_id_type=MESH,
        )

    pl.semaphore_wait(barrier, len(targets) + len(others))
    mark_copies, cache_copies = [], []
    for i, distance in enumerate(DISTANCES):
        copy = send(mark.at[i], mark_in.at[i], mark_sems, i, distance)
        copy.start()
        mark_copies.append(copy)
    for i, distance in enumerate(DISTANCES):
        for a in range(2):
            total = updated[a, 0] * flag(offset[0] == distance, (1, local))
            for c in range(1, spans):
                total = total + updated[a, c] * flag(offset[c] == distance, (1, local))
            parcel[i, a] = total
        copy = send(parcel.at[i], arrived.at[i], cache_sems, i, distance)
        copy.start()
        cache_copies.append(copy)

    for l in range(spans):
        for a in range(2):
            total = updated[a, 0] * flag((offset[0] == 0) & (place[0] == l), (1, local))
            for c in range(1, spans):
                keep = flag((offset[c] == 0) & (place[c] == l), (1, local))
                total = total + updated[a, c] * keep
            moved_cache[a, l] = total

    contexts = []
    for c in range(spans):
        query, key, value = (token_qkv[k, c : c + 1, :] for k in range(3))
        contexts.append(
            attend(query, self_cache[0, c], self_cache[1, c], cache_len[c], (key, value))
        )
    pad = part.shape[0] - spans
    context = jnp.concatenate(contexts + [jnp.zeros((pad, local), jnp.float32)], 0)
    context = context.astype(jnp.bfloat16)
    loads[0].wait()
    part[...] = jnp.dot(context, out_proj[...], preferred_element_type=jnp.float32)
    part_copies = []
    for k, other in enumerate(others):
        copy = pltpu.make_async_remote_copy(
            src_ref=part,
            dst_ref=part_in.at[k],
            send_sem=part_sems.at[0, k],
            recv_sem=part_sems.at[1, k],
            device_id={"mp": other},
            device_id_type=MESH,
        )
        copy.start()
        part_copies.append(copy)
    loads[1].wait()
    loads[2].wait()
    for copy in part_copies:
        copy.wait()
    summed = part[...]
    for k in range(len(others)):
        summed = summed + part_in[k]
    resid = hidden[...].astype(jnp.float32) + summed[:spans]
    centre = jnp.mean(resid, axis=-1, keepdims=True)
    spread = jnp.mean((resid - centre) ** 2, axis=-1, keepdims=True)
    gain = ln_gain[...].reshape(1, width)
    bias = ln_bias[...].reshape(1, width)
    normed = (resid - centre) * lax.rsqrt(spread + 1e-05) * gain + bias
    normed = jnp.concatenate([normed, jnp.zeros((pad, width), jnp.float32)], 0)
    query = jnp.dot(
        normed.astype(jnp.bfloat16), query_proj[...], preferred_element_type=jnp.float32
    ).astype(jnp.bfloat16).astype(jnp.float32)
    decoded = []
    for c in range(spans):
        mixed = attend(query[c : c + 1], cross[0, c], cross[1, c], None, None)
        decoded.append(mixed * jnp.where(alive[c] == 1, 1.0, 0.0))

    line_copies = []
    blank = jnp.zeros((line.shape[1] - 1, local), jnp.float32)
    for i, distance in enumerate(DISTANCES):
        row = jnp.zeros((1, local), jnp.float32)
        for c in range(spans):
            row = row + decoded[c] * jnp.where(offset[c] == distance, 1.0, 0.0)
        line[i] = jnp.concatenate([row, blank], 0).astype(jnp.bfloat16)
        copy = send(line.at[i], line_in.at[i], line_sems, i, distance)
        copy.start()
        line_copies.append(copy)

    rows = []
    for l in range(spans):
        row = jnp.zeros((1, local), jnp.float32)
        for c in range(spans):
            keep = (offset[c] == 0) & (place[c] == l)
            row = row + decoded[c] * jnp.where(keep, 1.0, 0.0)
        rows.append(row)
    for i in range(len(DISTANCES)):
        mark_copies[i].wait()
        cache_copies[i].wait()
        for l in range(spans):
            taken = mark_in[i, l : l + 1, :]
            for a in range(2):
                moved_cache[a, l] = moved_cache[a, l] + arrived[i, a] * taken
    for i in range(len(DISTANCES)):
        line_copies[i].wait()
        for l in range(spans):
            taken = mark_in[i, l : l + 1, :].astype(jnp.float32)
            rows[l] = rows[l] + line_in[i, 0:1, :].astype(jnp.float32) * taken
    moved_out[...] = jnp.concatenate(rows, 0).astype(jnp.bfloat16)


def relay_kernel(
    count,
    cores,
    cache_len,
    finished,
    new_slot,
    hidden,
    token_qkv,
    self_cache,
    ln_gain,
    ln_bias,
    cross_hbm,
    out_proj_hbm,
    query_proj_hbm,
    moved_cache,
    moved_out,
    cross,
    out_proj,
    query_proj,
    own,
    raw_in,
    cross_out,
    cross_in,
    kept,
    final_out,
    final_in,
    pick,
    label,
    label_in,
    line,
    line_in,
    part,
    part_in,
    load_sem,
    raw_send,
    raw_recv,
    hop_sems,
    label_send,
    label_recv,
    line_sems,
    part_sems,
):
    spans, width = hidden.shape
    slots, local = self_cache.shape[2:]
    steps, _, rows_per, _ = own.shape
    per = steps // 2
    me = lax.axis_index("batch")
    core = lax.axis_index("mp")
    level, column = lax.div(me, 2), lax.rem(me, 2)
    left = level < REACH - 1
    inner = (level == 1) | (level == REACH - 1)
    outer = jnp.logical_not(inner)
    loads = [
        pltpu.make_async_copy(source, target, load_sem.at[i])
        for i, (source, target) in enumerate(
            [(out_proj_hbm, out_proj), (query_proj_hbm, query_proj), (cross_hbm, cross)]
        )
    ]
    for load in loads:
        load.start()

    barrier = pltpu.get_barrier_semaphore()
    targets = [lax.rem(me + distance + count, count) for distance in DISTANCES]
    for target in targets:
        pl.semaphore_signal(barrier, inc=1, device_id={"batch": target}, device_id_type=MESH)
    others = [lax.rem(core + k, cores) for k in range(1, cores)]
    for other in others:
        pl.semaphore_signal(barrier, inc=1, device_id={"mp": other}, device_id_type=MESH)

    mate_level = jnp.where(level == 0, 1, jnp.where(level == 1, 0, jnp.where(level == 2, 3, 2)))
    mate = mate_level * 2 + column
    mate_aside = mate_level * 2 + 1 - column
    aside = level * 2 + 1 - column
    across = (REACH - level) * 2 + column
    beyond = (REACH - mate_level) * 2 + column

    half = count // 2
    alive, offset, place = [], [], []
    for c in range(spans):
        slot = new_slot[c]
        owner = lax.div(slot, spans)
        offset.append(lax.rem(owner - me + half + count, count) - half)
        place.append(lax.rem(slot, spans))
        alive.append(jnp.where(finished[c] == 0, 1, 0))

    def to(node, source, target, sent, received):
        return pltpu.make_async_remote_copy(
            src_ref=source,
            dst_ref=target,
            send_sem=sent,
            recv_sem=received,
            device_id={"batch": node},
            device_id_type=MESH,
        )

    def raw_copy(node, lane, way, k):
        return to(node, own.at[k], raw_in.at[way, k], raw_send.at[lane, k], raw_recv.at[way, k])

    def cross_copy(k):
        return to(across, cross_out.at[k], cross_in.at[k], hop_sems.at[0, k], hop_sems.at[1, k])

    def final_copy(k):
        return to(mate, final_out.at[k], final_in.at[k], hop_sems.at[2, k], hop_sems.at[3, k])

    def label_copy(node, lane, way):
        return to(node, label, label_in.at[way], label_send.at[lane], label_recv.at[way])

    def line_copy(i):
        return to(targets[i], line.at[i], line_in.at[i], line_sems.at[0, i], line_sems.at[1, i])

    label_row = lax.broadcasted_iota(jnp.int32, label.shape, 0)
    labels = jnp.zeros(label.shape, jnp.int32)
    for c in range(spans):
        labels = jnp.where(label_row == c, new_slot[c], labels)
    label[...] = labels.astype(jnp.float32)

    pl.semaphore_wait(barrier, len(targets) + len(others))

    position = lax.broadcasted_iota(jnp.int32, (rows_per, local), 0)
    ends = [cache_len[c] * alive[c] for c in range(spans)]
    fresh_at = [jnp.where(alive[c] == 1, cache_len[c], -1) for c in range(spans)]

    def grow(k, _):
        a, r = lax.div(k, per), lax.rem(k, per)
        start = pl.multiple_of(r * rows_per, rows_per)
        at = position + start
        for c in range(spans):
            older = jnp.where(at < ends[c], 1.0, 0.0).astype(jnp.bfloat16)
            fresh = jnp.where(at == fresh_at[c], 1.0, 0.0).astype(jnp.bfloat16)
            new = jnp.where(a == 0, token_qkv[1, c : c + 1, :].astype(jnp.float32),
                            token_qkv[2, c : c + 1, :].astype(jnp.float32)).astype(jnp.bfloat16)
            own[k, c] = self_cache[a, c, pl.ds(start, rows_per), :] * older + new * fresh

        @pl.when(outer)
        def _():
            raw_copy(mate, 0, 0, k).start()
            raw_copy(mate_aside, 1, 1, k).start()

        @pl.when(inner)
        def _():
            raw_copy(aside, 0, 2, k).start()

        return 0

    @pl.when(outer)
    def _():
        label_copy(mate, 0, 0).start()
        label_copy(mate_aside, 1, 1).start()

    @pl.when(inner)
    def _():
        label_copy(aside, 0, 2).start()

    lax.fori_loop(0, steps, grow, 0)

    def self_part():
        contexts = []
        for c in range(spans):
            query, key, value = (token_qkv[k, c : c + 1, :] for k in range(3))
            contexts.append(
                attend(query, self_cache[0, c], self_cache[1, c], cache_len[c], (key, value))
            )
        context = jnp.concatenate(contexts + [jnp.zeros((pad, local), jnp.float32)], 0)
        context = context.astype(jnp.bfloat16)
        loads[0].wait()
        part[...] = jnp.dot(context, out_proj[...], preferred_element_type=jnp.float32)

    def part_copy(k):
        return pltpu.make_async_remote_copy(
            src_ref=part,
            dst_ref=part_in.at[k],
            send_sem=part_sems.at[0, k],
            recv_sem=part_sems.at[1, k],
            device_id={"mp": others[k]},
            device_id_type=MESH,
        )

    pad = part.shape[0] - spans
    self_part()
    for k in range(len(others)):
        part_copy(k).start()

    @pl.when(inner)
    def _():
        for way in range(3):
            label_copy(mate, 0, way).wait_recv()
        sources = [label] + [label_in.at[way] for way in range(3)]
        nodes = [me, mate, across, beyond]
        for s, source in enumerate(sources):
            for c in range(spans):
                held = jnp.broadcast_to(source[c : c + 1, 0:1], (rows_per, local))
                for d, node in enumerate(nodes):
                    for l in range(spans):
                        wanted = jnp.full((rows_per, local), node * spans + l, jnp.int32)
                        pick[s * spans + c, d * spans + l] = jnp.where(
                            held == wanted.astype(jnp.float32), 1.0, 0.0
                        ).astype(jnp.bfloat16)

    def merge(k, _):
        for way in range(3):
            raw_copy(mate, 0, way, k).wait_recv()
        blocks = [own[k, c] for c in range(spans)]
        for way in range(3):
            blocks += [raw_in[way, k, c] for c in range(spans)]

        def gathered(d):
            total = blocks[0] * pick[0, d]
            for s in range(1, len(blocks)):
                total = total + blocks[s] * pick[s, d]
            return total

        for d in range(2 * spans):
            cross_out[k, d] = gathered(2 * spans + d)
        cross_copy(k).start()
        for d in range(2 * spans):
            kept[k, d] = gathered(d)
        return 0

    def finish(k, _):
        cross_copy(k).wait_recv()
        a, r = lax.div(k, per), lax.rem(k, per)
        start = pl.multiple_of(r * rows_per, rows_per)
        for l in range(spans):
            final_out[k, l] = kept[k, spans + l] + cross_in[k, spans + l]
        final_copy(k).start()
        for l in range(spans):
            moved_cache[a, l, pl.ds(start, rows_per), :] = kept[k, l] + cross_in[k, l]
        return 0

    def both(k, _):
        merge(k, 0)
        finish(k - LAG, 0)
        return 0

    @pl.when(inner)
    def _():
        lax.fori_loop(0, EARLY, merge, 0)

    loads[1].wait()
    loads[2].wait()
    for k in range(len(others)):
        part_copy(k).wait()
    summed = part[...]
    for k in range(len(others)):
        summed = summed + part_in[k]
    resid = hidden[...].astype(jnp.float32) + summed[:spans]
    centre = jnp.mean(resid, axis=-1, keepdims=True)
    spread = jnp.mean((resid - centre) ** 2, axis=-1, keepdims=True)
    gain = ln_gain[...].reshape(1, width)
    bias = ln_bias[...].reshape(1, width)
    normed = (resid - centre) * lax.rsqrt(spread + 1e-05) * gain + bias
    normed = jnp.concatenate([normed, jnp.zeros((pad, width), jnp.float32)], 0)
    query = jnp.dot(
        normed.astype(jnp.bfloat16), query_proj[...], preferred_element_type=jnp.float32
    ).astype(jnp.bfloat16).astype(jnp.float32)

    @pl.when(inner)
    def _():
        lax.fori_loop(EARLY, LAG, merge, 0)

    decoded = []
    for c in range(spans):
        mixed = attend(query[c : c + 1], cross[0, c], cross[1, c], None, None)
        decoded.append(mixed * jnp.where(alive[c] == 1, 1.0, 0.0))

    def placed(distance):
        rows = []
        for l in range(spans):
            row = jnp.zeros((1, local), jnp.float32)
            for c in range(spans):
                keep = (offset[c] == distance) & (place[c] == l)
                row = row + decoded[c] * jnp.where(keep, 1.0, 0.0)
            rows.append(row)
        return jnp.concatenate(rows, 0)

    for i, distance in enumerate(DISTANCES):
        line[i] = placed(distance).astype(jnp.bfloat16)
        line_copy(i).start()

    @pl.when(inner)
    def _():
        lax.fori_loop(LAG, steps, both, 0)

    total = placed(0)
    for i in range(len(DISTANCES)):
        line_copy(i).wait()
        total = total + line_in[i].astype(jnp.float32)
    moved_out[...] = total.astype(jnp.bfloat16)

    def land(k, _):
        final_copy(k).wait_recv()
        a, r = lax.div(k, per), lax.rem(k, per)
        start = pl.multiple_of(r * rows_per, rows_per)
        for l in range(spans):
            moved_cache[a, l, pl.ds(start, rows_per), :] = final_in[k, l]
        return 0

    def outer_sent(k, _):
        raw_copy(mate, 0, 0, k).wait_send()
        raw_copy(mate_aside, 1, 1, k).wait_send()
        return 0

    def inner_sent(k, _):
        raw_copy(aside, 0, 2, k).wait_send()
        cross_copy(k).wait_send()
        final_copy(k).wait_send()
        return 0

    @pl.when(inner)
    def _():
        lax.fori_loop(steps - LAG, steps, finish, 0)
        label_copy(aside, 0, 2).wait_send()
        lax.fori_loop(0, steps, inner_sent, 0)

    @pl.when(outer)
    def _():
        lax.fori_loop(0, steps, land, 0)
        label_copy(mate, 0, 0).wait_send()
        label_copy(mate_aside, 1, 1).wait_send()
        lax.fori_loop(0, steps, outer_sent, 0)


def body(
    hidden,
    token_qkv,
    self_cache,
    cross_kv,
    cache_len,
    finished,
    new_slot,
    out_proj,
    ln_gain,
    ln_bias,
    query_proj,
):
    count, cores = lax.axis_size("batch"), lax.axis_size("mp")
    spans, width = hidden.shape
    slots, local = self_cache.shape[2:]
    moves = len(DISTANCES)
    smem = pl.BlockSpec(memory_space=pltpu.SMEM)
    vmem = pl.BlockSpec(memory_space=pltpu.VMEM)
    away = pl.BlockSpec(memory_space=pl.ANY)
    bf16, f32 = jnp.bfloat16, jnp.float32
    operands = (
        cache_len,
        finished,
        new_slot,
        hidden,
        token_qkv,
        self_cache,
        ln_gain,
        ln_bias,
        cross_kv,
        out_proj,
        query_proj,
    )
    parcels = pltpu.VMEM((moves, 2, slots, local), bf16)
    tiles = pltpu.VMEM((moves, 16, local), bf16)
    dma = pltpu.SemaphoreType.DMA
    inputs = [pltpu.VMEM(array.shape, bf16) for array in (cross_kv, out_proj, query_proj)]
    parts = [pltpu.VMEM((8, width), f32), pltpu.VMEM((cores - 1, 8, width), f32)]
    steps = 2 * slots // ROWS
    if count == 2 * (REACH + 1):
        function = relay_kernel

        def blocks(*lead):
            return pltpu.VMEM(lead + (ROWS, local), bf16)

        scratch = inputs + [
            blocks(steps, spans),
            blocks(3, steps, spans),
            blocks(steps, 2 * spans),
            blocks(steps, 2 * spans),
            blocks(steps, 2 * spans),
            blocks(steps, spans),
            blocks(steps, spans),
            blocks(4 * spans, 4 * spans),
            pltpu.VMEM((8, 128), f32),
            pltpu.VMEM((3, 8, 128), f32),
            pltpu.VMEM((moves, spans, local), bf16),
            pltpu.VMEM((moves, spans, local), bf16),
            *parts,
            dma((3,)),
            dma((2, steps)),
            dma((3, steps)),
            dma((4, steps)),
            dma((2,)),
            dma((3,)),
            dma((2, moves)),
            dma((2, cores - 1)),
        ]
    else:
        function = kernel
        scratch = inputs + [
            pltpu.VMEM(self_cache.shape, bf16),
            parcels,
            parcels,
            tiles,
            tiles,
            tiles,
            tiles,
            *parts,
            dma((3,)),
            dma((2, moves)),
            dma((2, moves)),
            dma((2, moves)),
            dma((2, cores - 1)),
        ]
    return pl.pallas_call(
        functools.partial(function, count, cores),
        out_shape=(
            jax.ShapeDtypeStruct(self_cache.shape, bf16),
            jax.ShapeDtypeStruct((spans, local), bf16),
        ),
        in_specs=[smem] * 3 + [vmem] * 5 + [away] * 3,
        out_specs=(vmem, vmem),
        scratch_shapes=scratch,
        compiler_params=pltpu.CompilerParams(collective_id=0, has_side_effects=True),
    )(*operands)


def solution(mesh):
    placed = (
        P(("groups", "batch"), None),
        P(None, ("groups", "batch"), "mp"),
        P(None, ("groups", "batch"), None, "mp"),
        P(None, ("groups", "batch"), None, "mp"),
        P(("groups", "batch")),
        P(("groups", "batch")),
        P(("groups", "batch")),
        P("mp", None),
        P(),
        P(),
        P(None, "mp"),
    )
    return jax.shard_map(
        body,
        mesh=mesh,
        in_specs=placed,
        out_specs=(P(None, ("groups", "batch"), None, "mp"), P(("groups", "batch"), "mp")),
        check_vma=False,
    )
```

```python
import functools

import jax
import jax.numpy as jnp
from jax import lax
from jax.experimental import pallas as pl
from jax.experimental.pallas import tpu as pltpu
from jax.sharding import PartitionSpec as P

HEAD_DIM = 64
REACH = 3
MESH = pl.DeviceIdType.MESH
DISTANCES = [3, -3, 2, -2, 1, -1]
ROWS = 16
LAG = 3
EARLY = 1
MIDDLE = 14
HOLD = 8


def attend(query, keys, values, length, own):
    slots, width = keys.shape
    heads = width // HEAD_DIM
    rows = -(-heads // 16) * 16
    row = lax.broadcasted_iota(jnp.int32, (rows, width), 0)
    column = lax.broadcasted_iota(jnp.int32, (rows, width), 1)
    low = row * HEAD_DIM
    mine = (column >= low) & (column < low + HEAD_DIM)
    spread = jnp.where(mine, query.astype(jnp.float32), 0.0)
    factor = HEAD_DIM ** (-0.5)
    scores = (
        lax.dot_general(
            spread.astype(jnp.bfloat16),
            keys,
            (((1,), (1,)), ((), ())),
            preferred_element_type=jnp.float32,
        )
        * factor
    )
    if length is not None:
        usable = lax.broadcasted_iota(jnp.int32, (rows, slots), 1) < length
        scores = jnp.where(usable, scores, -1e30)
    highest = jnp.max(scores, axis=-1, keepdims=True)
    if own is not None:
        new_key, new_value = own
        own_score = jnp.sum(spread * new_key.astype(jnp.float32), axis=-1, keepdims=True) * factor
        highest = jnp.maximum(highest, own_score)
    weight = jnp.exp(scores - highest)
    if length is not None:
        weight = jnp.where(usable, weight, 0.0)
    total = jnp.sum(weight, axis=-1, keepdims=True)
    if own is not None:
        own_weight = jnp.exp(own_score - highest)
        total = total + own_weight
    weight = (weight / total).astype(jnp.bfloat16)
    mixed = jnp.dot(weight, values, preferred_element_type=jnp.float32)
    if own is not None:
        own_weight = (own_weight / total).astype(jnp.bfloat16).astype(jnp.float32)
        mixed = mixed + own_weight * new_value.astype(jnp.float32)
    return jnp.sum(jnp.where(mine, mixed, 0.0), axis=0, keepdims=True)


def kernel(
    count,
    cores,
    cache_len,
    finished,
    new_slot,
    hidden,
    token_qkv,
    self_cache,
    ln_gain,
    ln_bias,
    cross_hbm,
    out_proj_hbm,
    query_proj_hbm,
    moved_cache,
    moved_out,
    cross,
    out_proj,
    query_proj,
    updated,
    parcel,
    arrived,
    mark,
    mark_in,
    line,
    line_in,
    part,
    part_in,
    load_sem,
    cache_sems,
    mark_sems,
    line_sems,
    part_sems,
):
    spans, width = hidden.shape
    slots, local = self_cache.shape[2:]
    me = lax.axis_index("batch")
    core = lax.axis_index("mp")
    loads = [
        pltpu.make_async_copy(source, target, load_sem.at[i])
        for i, (source, target) in enumerate(
            [(out_proj_hbm, out_proj), (query_proj_hbm, query_proj), (cross_hbm, cross)]
        )
    ]
    for load in loads:
        load.start()

    barrier = pltpu.get_barrier_semaphore()
    targets = [lax.rem(me + distance + count, count) for distance in DISTANCES]
    for target in targets:
        pl.semaphore_signal(barrier, inc=1, device_id={"batch": target}, device_id_type=MESH)
    others = [lax.rem(core + k, cores) for k in range(1, cores)]
    for other in others:
        pl.semaphore_signal(barrier, inc=1, device_id={"mp": other}, device_id_type=MESH)

    half = count // 2
    alive, offset, place = [], [], []
    for c in range(spans):
        slot = new_slot[c]
        owner = lax.div(slot, spans)
        offset.append(lax.rem(owner - me + half + count, count) - half)
        place.append(lax.rem(slot, spans))
        alive.append(jnp.where(finished[c] == 0, 1, 0))

    position = lax.broadcasted_iota(jnp.int32, (slots, local), 0)
    for c in range(spans):
        length = cache_len[c]
        older = jnp.where(position < length * alive[c], 1.0, 0.0).astype(jnp.bfloat16)
        fresh = jnp.where(position == jnp.where(alive[c] == 1, length, -1), 1.0, 0.0).astype(
            jnp.bfloat16
        )
        for a in range(2):
            updated[a, c] = self_cache[a, c] * older + token_qkv[1 + a, c : c + 1, :] * fresh

    def flag(value, shape):
        return jnp.full(shape, jnp.where(value, 1.0, 0.0), jnp.float32).astype(jnp.bfloat16)

    marker_row = lax.broadcasted_iota(jnp.int32, mark.shape[1:], 0)
    for i, distance in enumerate(DISTANCES):
        marker = jnp.zeros(mark.shape[1:], jnp.float32)
        for c in range(spans):
            at = jnp.where(offset[c] == distance, place[c], -1)
            marker = jnp.where(marker_row == at, 1.0, marker)
        mark[i] = marker.astype(jnp.bfloat16)

    def send(source, target, sems, i, distance):
        return pltpu.make_async_remote_copy(
            src_ref=source,
            dst_ref=target,
            send_sem=sems.at[0, i],
            recv_sem=sems.at[1, i],
            device_id={"batch": targets[i]},
            device_id_type=MESH,
        )

    pl.semaphore_wait(barrier, len(targets) + len(others))
    mark_copies, cache_copies = [], []
    for i, distance in enumerate(DISTANCES):
        copy = send(mark.at[i], mark_in.at[i], mark_sems, i, distance)
        copy.start()
        mark_copies.append(copy)
    for i, distance in enumerate(DISTANCES):
        for a in range(2):
            total = updated[a, 0] * flag(offset[0] == distance, (1, local))
            for c in range(1, spans):
                total = total + updated[a, c] * flag(offset[c] == distance, (1, local))
            parcel[i, a] = total
        copy = send(parcel.at[i], arrived.at[i], cache_sems, i, distance)
        copy.start()
        cache_copies.append(copy)

    for l in range(spans):
        for a in range(2):
            total = updated[a, 0] * flag((offset[0] == 0) & (place[0] == l), (1, local))
            for c in range(1, spans):
                keep = flag((offset[c] == 0) & (place[c] == l), (1, local))
                total = total + updated[a, c] * keep
            moved_cache[a, l] = total

    contexts = []
    for c in range(spans):
        query, key, value = (token_qkv[k, c : c + 1, :] for k in range(3))
        contexts.append(
            attend(query, self_cache[0, c], self_cache[1, c], cache_len[c], (key, value))
        )
    pad = part.shape[0] - spans
    context = jnp.concatenate(contexts + [jnp.zeros((pad, local), jnp.float32)], 0)
    context = context.astype(jnp.bfloat16)
    loads[0].wait()
    part[...] = jnp.dot(context, out_proj[...], preferred_element_type=jnp.float32)
    part_copies = []
    for k, other in enumerate(others):
        copy = pltpu.make_async_remote_copy(
            src_ref=part,
            dst_ref=part_in.at[k],
            send_sem=part_sems.at[0, k],
            recv_sem=part_sems.at[1, k],
            device_id={"mp": other},
            device_id_type=MESH,
        )
        copy.start()
        part_copies.append(copy)
    loads[1].wait()
    loads[2].wait()
    for copy in part_copies:
        copy.wait()
    summed = part[...]
    for k in range(len(others)):
        summed = summed + part_in[k]
    resid = hidden[...].astype(jnp.float32) + summed[:spans]
    centre = jnp.mean(resid, axis=-1, keepdims=True)
    spread = jnp.mean((resid - centre) ** 2, axis=-1, keepdims=True)
    gain = ln_gain[...].reshape(1, width)
    bias = ln_bias[...].reshape(1, width)
    normed = (resid - centre) * lax.rsqrt(spread + 1e-05) * gain + bias
    normed = jnp.concatenate([normed, jnp.zeros((pad, width), jnp.float32)], 0)
    query = jnp.dot(
        normed.astype(jnp.bfloat16), query_proj[...], preferred_element_type=jnp.float32
    ).astype(jnp.bfloat16).astype(jnp.float32)
    decoded = []
    for c in range(spans):
        mixed = attend(query[c : c + 1], cross[0, c], cross[1, c], None, None)
        decoded.append(mixed * jnp.where(alive[c] == 1, 1.0, 0.0))

    line_copies = []
    blank = jnp.zeros((line.shape[1] - 1, local), jnp.float32)
    for i, distance in enumerate(DISTANCES):
        row = jnp.zeros((1, local), jnp.float32)
        for c in range(spans):
            row = row + decoded[c] * jnp.where(offset[c] == distance, 1.0, 0.0)
        line[i] = jnp.concatenate([row, blank], 0).astype(jnp.bfloat16)
        copy = send(line.at[i], line_in.at[i], line_sems, i, distance)
        copy.start()
        line_copies.append(copy)

    rows = []
    for l in range(spans):
        row = jnp.zeros((1, local), jnp.float32)
        for c in range(spans):
            keep = (offset[c] == 0) & (place[c] == l)
            row = row + decoded[c] * jnp.where(keep, 1.0, 0.0)
        rows.append(row)
    for i in range(len(DISTANCES)):
        mark_copies[i].wait()
        cache_copies[i].wait()
        for l in range(spans):
            taken = mark_in[i, l : l + 1, :]
            for a in range(2):
                moved_cache[a, l] = moved_cache[a, l] + arrived[i, a] * taken
    for i in range(len(DISTANCES)):
        line_copies[i].wait()
        for l in range(spans):
            taken = mark_in[i, l : l + 1, :].astype(jnp.float32)
            rows[l] = rows[l] + line_in[i, 0:1, :].astype(jnp.float32) * taken
    moved_out[...] = jnp.concatenate(rows, 0).astype(jnp.bfloat16)


def relay_kernel(
    count,
    cores,
    cache_len,
    finished,
    new_slot,
    hidden,
    token_qkv,
    cache_hbm,
    ln_gain,
    ln_bias,
    cross_hbm,
    out_proj_hbm,
    query_proj_hbm,
    moved_cache,
    moved_out,
    self_cache,
    cross,
    out_proj,
    query_proj,
    own,
    raw_in,
    cross_out,
    cross_in,
    kept,
    final_out,
    final_in,
    pick,
    label,
    label_in,
    line,
    line_in,
    line_kept,
    line_out,
    line_cross,
    line_last,
    line_final,
    part,
    part_in,
    load_sem,
    raw_send,
    raw_recv,
    hop_sems,
    label_send,
    label_recv,
    line_send,
    line_recv,
    line_hops,
    part_sems,
):
    spans, width = hidden.shape
    slots, local = self_cache.shape[2:]
    steps, _, rows_per, _ = own.shape
    per = steps // 2
    me = lax.axis_index("batch")
    core = lax.axis_index("mp")
    level, column = lax.div(me, 2), lax.rem(me, 2)
    inner = (level == 1) | (level == REACH - 1)
    outer = jnp.logical_not(inner)
    barrier = pltpu.get_barrier_semaphore()

    def greet(where):
        pl.semaphore_signal(barrier, inc=1, device_id=where, device_id_type=MESH)

    mate_level = jnp.where(level == 0, 1, jnp.where(level == 1, 0, jnp.where(level == 2, 3, 2)))
    mate = mate_level * 2 + column
    mate_aside = mate_level * 2 + 1 - column
    aside = level * 2 + 1 - column
    across = (REACH - level) * 2 + column
    beyond = (REACH - mate_level) * 2 + column
    others = [lax.rem(core + k, cores) for k in range(1, cores)]
    for node in (mate, mate_aside):
        greet({"batch": node})

    @pl.when(inner)
    def _():
        greet({"batch": aside})
        greet({"batch": across})

    for other in others:
        greet({"mp": other})
    loads = [
        pltpu.make_async_copy(source, target, load_sem.at[i])
        for i, (source, target) in enumerate(
            [
                (out_proj_hbm, out_proj),
                (query_proj_hbm, query_proj),
                (cross_hbm, cross),
                (cache_hbm.at[0], self_cache.at[0]),
                (cache_hbm.at[1], self_cache.at[1]),
            ]
        )
    ]
    for i in (3, 4, 0, 1, 2):
        loads[i].start()

    alive = [jnp.where(finished[c] == 0, 1, 0) for c in range(spans)]

    def to(node, source, target, sent, received):
        return pltpu.make_async_remote_copy(
            src_ref=source,
            dst_ref=target,
            send_sem=sent,
            recv_sem=received,
            device_id={"batch": node},
            device_id_type=MESH,
        )

    def raw_copy(node, lane, way, k):
        return to(node, own.at[k], raw_in.at[way, k], raw_send.at[lane, k], raw_recv.at[way, k])

    def cross_copy(k, part):
        first = (1 - part) * spans
        return to(
            across,
            cross_out.at[k, pl.ds(first, spans)],
            cross_in.at[k, pl.ds(first, spans)],
            hop_sems.at[2 * part, k],
            hop_sems.at[2 * part + 1, k],
        )

    def final_copy(k):
        return to(mate, final_out.at[k], final_in.at[k], hop_sems.at[4, k], hop_sems.at[5, k])

    def label_copy(node, lane, way):
        return to(node, label, label_in.at[way], label_send.at[lane], label_recv.at[way])

    def line_copy(node, lane, way):
        return to(node, line, line_in.at[way], line_send.at[lane], line_recv.at[way])

    def line_cross_copy():
        return to(across, line_out, line_cross, line_hops.at[0], line_hops.at[1])

    def line_final_copy():
        return to(mate, line_last, line_final, line_hops.at[2], line_hops.at[3])

    label_row = lax.broadcasted_iota(jnp.int32, label.shape, 0)
    labels = jnp.zeros(label.shape, jnp.int32)
    for c in range(spans):
        labels = jnp.where(label_row == c, new_slot[c], labels)
    label[...] = labels.astype(jnp.float32)

    @pl.when(inner)
    def _():
        pl.semaphore_wait(barrier, 4 + len(others))

    @pl.when(outer)
    def _():
        pl.semaphore_wait(barrier, 2 + len(others))

    position = lax.broadcasted_iota(jnp.int32, (rows_per, local), 0)
    ends = [cache_len[c] * alive[c] for c in range(spans)]
    fresh_at = [jnp.where(alive[c] == 1, cache_len[c], -1) for c in range(spans)]

    def grow(k, _):
        a, r = lax.div(k, per), lax.rem(k, per)
        start = pl.multiple_of(r * rows_per, rows_per)
        at = position + start
        for c in range(spans):
            older = jnp.where(at < ends[c], 1.0, 0.0).astype(jnp.bfloat16)
            fresh = jnp.where(at == fresh_at[c], 1.0, 0.0).astype(jnp.bfloat16)
            new = jnp.where(a == 0, token_qkv[1, c : c + 1, :].astype(jnp.float32),
                            token_qkv[2, c : c + 1, :].astype(jnp.float32)).astype(jnp.bfloat16)
            own[k, c] = self_cache[a, c, pl.ds(start, rows_per), :] * older + new * fresh

        return 0

    def pass_on(k, _):
        @pl.when(outer)
        def _():
            raw_copy(mate, 0, 0, k).start()
            raw_copy(mate_aside, 1, 1, k).start()

        @pl.when(inner)
        def _():
            raw_copy(aside, 0, 2, k).start()

        return 0

    def grow_and_pass(k, _):
        grow(k, 0)
        pass_on(k, 0)
        return 0

    @pl.when(outer)
    def _():
        label_copy(mate, 0, 0).start()
        label_copy(mate_aside, 1, 1).start()

    @pl.when(inner)
    def _():
        label_copy(aside, 0, 2).start()

    loads[3].wait()
    lax.fori_loop(0, per, grow_and_pass, 0)
    loads[4].wait()
    lax.fori_loop(per, HOLD, grow_and_pass, 0)
    lax.fori_loop(HOLD, steps, grow, 0)

    def self_part():
        contexts = []
        for c in range(spans):
            query, key, value = (token_qkv[k, c : c + 1, :] for k in range(3))
            contexts.append(
                attend(query, self_cache[0, c], self_cache[1, c], cache_len[c], (key, value))
            )
        context = jnp.concatenate(contexts + [jnp.zeros((pad, local), jnp.float32)], 0)
        context = context.astype(jnp.bfloat16)
        loads[0].wait()
        part[...] = jnp.dot(context, out_proj[...], preferred_element_type=jnp.float32)

    def part_copy(k):
        return pltpu.make_async_remote_copy(
            src_ref=part,
            dst_ref=part_in.at[k],
            send_sem=part_sems.at[0, k],
            recv_sem=part_sems.at[1, k],
            device_id={"mp": others[k]},
            device_id_type=MESH,
        )

    pad = part.shape[0] - spans
    self_part()
    for k in range(len(others)):
        part_copy(k).start()

    @pl.when(inner)
    def _():
        for way in range(3):
            label_copy(mate, 0, way).wait_recv()
        sources = [label] + [label_in.at[way] for way in range(3)]
        nodes = [me, mate, across, beyond]
        for s, source in enumerate(sources):
            for c in range(spans):
                held = jnp.broadcast_to(source[c : c + 1, 0:1], (rows_per, local))
                for d, node in enumerate(nodes):
                    for l in range(spans):
                        wanted = jnp.full((rows_per, local), node * spans + l, jnp.int32)
                        pick[s * spans + c, d * spans + l] = jnp.where(
                            held == wanted.astype(jnp.float32), 1.0, 0.0
                        ).astype(jnp.bfloat16)

    def merge(k, _):
        for way in range(3):
            raw_copy(mate, 0, way, k).wait_recv()
        blocks = [own[k, c] for c in range(spans)]
        for way in range(3):
            blocks += [raw_in[way, k, c] for c in range(spans)]

        def gathered(d):
            total = blocks[0] * pick[0, d]
            for s in range(1, len(blocks)):
                total = total + blocks[s] * pick[s, d]
            return total

        for part in range(2):
            for d in range((1 - part) * spans, (2 - part) * spans):
                cross_out[k, d] = gathered(2 * spans + d)
            cross_copy(k, part).start()
        for d in range(2 * spans):
            kept[k, d] = gathered(d)
        return 0

    def finish(k, _):
        cross_copy(k, 0).wait_recv()
        a, r = lax.div(k, per), lax.rem(k, per)
        start = pl.multiple_of(r * rows_per, rows_per)
        for l in range(spans):
            final_out[k, l] = kept[k, spans + l] + cross_in[k, spans + l]
        final_copy(k).start()
        cross_copy(k, 1).wait_recv()
        for l in range(spans):
            moved_cache[a, l, pl.ds(start, rows_per), :] = kept[k, l] + cross_in[k, l]
        return 0

    def both(k, _):
        merge(k, 0)
        finish(k - LAG, 0)
        return 0

    @pl.when(inner)
    def _():
        lax.fori_loop(0, EARLY, merge, 0)

    loads[1].wait()
    loads[2].wait()
    for k in range(len(others)):
        part_copy(k).wait()
    summed = part[...]
    for k in range(len(others)):
        summed = summed + part_in[k]
    resid = hidden[...].astype(jnp.float32) + summed[:spans]
    centre = jnp.mean(resid, axis=-1, keepdims=True)
    spread = jnp.mean((resid - centre) ** 2, axis=-1, keepdims=True)
    gain = ln_gain[...].reshape(1, width)
    bias = ln_bias[...].reshape(1, width)
    normed = (resid - centre) * lax.rsqrt(spread + 1e-05) * gain + bias
    normed = jnp.concatenate([normed, jnp.zeros((pad, width), jnp.float32)], 0)
    query = jnp.dot(
        normed.astype(jnp.bfloat16), query_proj[...], preferred_element_type=jnp.float32
    ).astype(jnp.bfloat16).astype(jnp.float32)

    @pl.when(inner)
    def _():
        lax.fori_loop(EARLY, LAG, merge, 0)

    decoded = []
    for c in range(spans):
        mixed = attend(query[c : c + 1], cross[0, c], cross[1, c], None, None)
        decoded.append(mixed * jnp.where(alive[c] == 1, 1.0, 0.0))

    line[...] = jnp.concatenate(decoded, 0).astype(jnp.bfloat16)

    @pl.when(outer)
    def _():
        line_copy(mate, 0, 0).start()
        line_copy(mate_aside, 1, 1).start()

    @pl.when(inner)
    def _():
        line_copy(aside, 0, 2).start()

    lax.fori_loop(HOLD, steps, pass_on, 0)

    @pl.when(inner)
    def _():
        lax.fori_loop(LAG, MIDDLE, both, 0)
        for way in range(3):
            line_copy(mate, 0, way).wait_recv()
        blocks = []
        for held in [line] + [line_in.at[way] for way in range(3)]:
            blocks += [held[c : c + 1, :].astype(jnp.float32) for c in range(spans)]
        rows = []
        for d in range(4 * spans):
            total = blocks[0] * pick[0, d, 0:1, :].astype(jnp.float32)
            for s in range(1, len(blocks)):
                total = total + blocks[s] * pick[s, d, 0:1, :].astype(jnp.float32)
            rows.append(total)
        line_out[...] = jnp.concatenate(rows[2 * spans :], 0).astype(jnp.bfloat16)
        line_cross_copy().start()
        line_kept[...] = jnp.concatenate(rows[: 2 * spans], 0)
        lax.fori_loop(MIDDLE, steps, both, 0)
        line_cross_copy().wait_recv()
        total = line_kept[...] + line_cross[...].astype(jnp.float32)
        line_last[...] = total[spans:].astype(jnp.bfloat16)
        line_final_copy().start()
        moved_out[...] = total[:spans].astype(jnp.bfloat16)

    def land(k, _):
        final_copy(k).wait_recv()
        a, r = lax.div(k, per), lax.rem(k, per)
        start = pl.multiple_of(r * rows_per, rows_per)
        for l in range(spans):
            moved_cache[a, l, pl.ds(start, rows_per), :] = final_in[k, l]
        return 0

    def outer_sent(k, _):
        raw_copy(mate, 0, 0, k).wait_send()
        raw_copy(mate_aside, 1, 1, k).wait_send()
        return 0

    def inner_sent(k, _):
        raw_copy(aside, 0, 2, k).wait_send()
        cross_copy(k, 0).wait_send()
        cross_copy(k, 1).wait_send()
        final_copy(k).wait_send()
        return 0

    @pl.when(inner)
    def _():
        lax.fori_loop(steps - LAG, steps, finish, 0)
        label_copy(aside, 0, 2).wait_send()
        line_copy(aside, 0, 2).wait_send()
        line_cross_copy().wait_send()
        line_final_copy().wait_send()
        lax.fori_loop(0, steps, inner_sent, 0)

    @pl.when(outer)
    def _():
        lax.fori_loop(0, steps, land, 0)
        label_copy(mate, 0, 0).wait_send()
        label_copy(mate_aside, 1, 1).wait_send()
        line_copy(mate, 0, 0).wait_send()
        line_copy(mate_aside, 1, 1).wait_send()
        line_final_copy().wait_recv()
        moved_out[...] = line_final[...]
        lax.fori_loop(0, steps, outer_sent, 0)


def body(
    hidden,
    token_qkv,
    self_cache,
    cross_kv,
    cache_len,
    finished,
    new_slot,
    out_proj,
    ln_gain,
    ln_bias,
    query_proj,
):
    count, cores = lax.axis_size("batch"), lax.axis_size("mp")
    spans, width = hidden.shape
    slots, local = self_cache.shape[2:]
    moves = len(DISTANCES)
    smem = pl.BlockSpec(memory_space=pltpu.SMEM)
    vmem = pl.BlockSpec(memory_space=pltpu.VMEM)
    away = pl.BlockSpec(memory_space=pl.ANY)
    bf16, f32 = jnp.bfloat16, jnp.float32
    operands = (
        cache_len,
        finished,
        new_slot,
        hidden,
        token_qkv,
        self_cache,
        ln_gain,
        ln_bias,
        cross_kv,
        out_proj,
        query_proj,
    )
    parcels = pltpu.VMEM((moves, 2, slots, local), bf16)
    tiles = pltpu.VMEM((moves, 16, local), bf16)
    dma = pltpu.SemaphoreType.DMA
    inputs = [pltpu.VMEM(array.shape, bf16) for array in (cross_kv, out_proj, query_proj)]
    parts = [pltpu.VMEM((8, width), f32), pltpu.VMEM((cores - 1, 8, width), f32)]
    steps = 2 * slots // ROWS
    if count == 2 * (REACH + 1):
        function, cache_spec = relay_kernel, away

        def blocks(*lead):
            return pltpu.VMEM(lead + (ROWS, local), bf16)

        scratch = [pltpu.VMEM(self_cache.shape, bf16)] + inputs + [
            blocks(steps, spans),
            blocks(3, steps, spans),
            blocks(steps, 2 * spans),
            blocks(steps, 2 * spans),
            blocks(steps, 2 * spans),
            blocks(steps, spans),
            blocks(steps, spans),
            blocks(4 * spans, 4 * spans),
            pltpu.VMEM((8, 128), f32),
            pltpu.VMEM((3, 8, 128), f32),
            pltpu.VMEM((spans, local), bf16),
            pltpu.VMEM((3, spans, local), bf16),
            pltpu.VMEM((2 * spans, local), f32),
            pltpu.VMEM((2 * spans, local), bf16),
            pltpu.VMEM((2 * spans, local), bf16),
            pltpu.VMEM((spans, local), bf16),
            pltpu.VMEM((spans, local), bf16),
            *parts,
            dma((5,)),
            dma((2, steps)),
            dma((3, steps)),
            dma((6, steps)),
            dma((2,)),
            dma((3,)),
            dma((2,)),
            dma((3,)),
            dma((4,)),
            dma((2, cores - 1)),
        ]
    else:
        function, cache_spec = kernel, vmem
        scratch = inputs + [
            pltpu.VMEM(self_cache.shape, bf16),
            parcels,
            parcels,
            tiles,
            tiles,
            tiles,
            tiles,
            *parts,
            dma((3,)),
            dma((2, moves)),
            dma((2, moves)),
            dma((2, moves)),
            dma((2, cores - 1)),
        ]
    return pl.pallas_call(
        functools.partial(function, count, cores),
        out_shape=(
            pltpu.VMEM(self_cache.shape, bf16),
            pltpu.VMEM((spans, local), bf16),
        ),
        in_specs=[smem] * 3 + [vmem] * 2 + [cache_spec] + [vmem] * 2 + [away] * 3,
        out_specs=(vmem, vmem),
        scratch_shapes=scratch,
        compiler_params=pltpu.CompilerParams(collective_id=0, has_side_effects=True),
    )(*operands)


def solution(mesh):
    placed = (
        P(("groups", "batch"), None),
        P(None, ("groups", "batch"), "mp"),
        P(None, ("groups", "batch"), None, "mp"),
        P(None, ("groups", "batch"), None, "mp"),
        P(("groups", "batch")),
        P(("groups", "batch")),
        P(("groups", "batch")),
        P("mp", None),
        P(),
        P(),
        P(None, "mp"),
    )
    return jax.shard_map(
        body,
        mesh=mesh,
        in_specs=placed,
        out_specs=(P(None, ("groups", "batch"), None, "mp"), P(("groups", "batch"), "mp")),
        check_vma=False,
    )
```

```python
import functools

import jax
import jax.numpy as jnp
from jax import lax
from jax.experimental import pallas as pl
from jax.experimental.pallas import tpu as pltpu
from jax.sharding import PartitionSpec as P

HEAD_DIM = 64
REACH = 3
MESH = pl.DeviceIdType.MESH
DISTANCES = [3, -3, 2, -2, 1, -1]
ROWS = 16
LAG = 3
EARLY = 1
MIDDLE = 14
HOLD = 8


def attend(query, keys, values, length, own):
    slots, width = keys.shape
    heads = width // HEAD_DIM
    rows = -(-heads // 16) * 16
    row = lax.broadcasted_iota(jnp.int32, (rows, width), 0)
    column = lax.broadcasted_iota(jnp.int32, (rows, width), 1)
    low = row * HEAD_DIM
    mine = (column >= low) & (column < low + HEAD_DIM)
    spread = jnp.where(mine, query.astype(jnp.float32), 0.0)
    factor = HEAD_DIM ** (-0.5)
    scores = (
        lax.dot_general(
            spread.astype(jnp.bfloat16),
            keys,
            (((1,), (1,)), ((), ())),
            preferred_element_type=jnp.float32,
        )
        * factor
    )
    if length is not None:
        usable = lax.broadcasted_iota(jnp.int32, (rows, slots), 1) < length
        scores = jnp.where(usable, scores, -1e30)
    highest = jnp.max(scores, axis=-1, keepdims=True)
    if own is not None:
        new_key, new_value = own
        own_score = jnp.sum(spread * new_key.astype(jnp.float32), axis=-1, keepdims=True) * factor
        highest = jnp.maximum(highest, own_score)
    weight = jnp.exp(scores - highest)
    if length is not None:
        weight = jnp.where(usable, weight, 0.0)
    total = jnp.sum(weight, axis=-1, keepdims=True)
    if own is not None:
        own_weight = jnp.exp(own_score - highest)
        total = total + own_weight
    weight = (weight / total).astype(jnp.bfloat16)
    mixed = jnp.dot(weight, values, preferred_element_type=jnp.float32)
    if own is not None:
        own_weight = (own_weight / total).astype(jnp.bfloat16).astype(jnp.float32)
        mixed = mixed + own_weight * new_value.astype(jnp.float32)
    return jnp.sum(jnp.where(mine, mixed, 0.0), axis=0, keepdims=True)


def kernel(
    count,
    cores,
    cache_len,
    finished,
    new_slot,
    hidden,
    token_qkv,
    self_cache,
    ln_gain,
    ln_bias,
    cross_hbm,
    out_proj_hbm,
    query_proj_hbm,
    moved_cache,
    moved_out,
    cross,
    out_proj,
    query_proj,
    updated,
    parcel,
    arrived,
    mark,
    mark_in,
    line,
    line_in,
    part,
    part_in,
    load_sem,
    cache_sems,
    mark_sems,
    line_sems,
    part_sems,
):
    spans, width = hidden.shape
    slots, local = self_cache.shape[2:]
    me = lax.axis_index("batch")
    core = lax.axis_index("mp")
    loads = [
        pltpu.make_async_copy(source, target, load_sem.at[i])
        for i, (source, target) in enumerate(
            [(out_proj_hbm, out_proj), (query_proj_hbm, query_proj), (cross_hbm, cross)]
        )
    ]
    for load in loads:
        load.start()

    barrier = pltpu.get_barrier_semaphore()
    targets = [lax.rem(me + distance + count, count) for distance in DISTANCES]
    for target in targets:
        pl.semaphore_signal(barrier, inc=1, device_id={"batch": target}, device_id_type=MESH)
    others = [lax.rem(core + k, cores) for k in range(1, cores)]
    for other in others:
        pl.semaphore_signal(barrier, inc=1, device_id={"mp": other}, device_id_type=MESH)

    half = count // 2
    alive, offset, place = [], [], []
    for c in range(spans):
        slot = new_slot[c]
        owner = lax.div(slot, spans)
        offset.append(lax.rem(owner - me + half + count, count) - half)
        place.append(lax.rem(slot, spans))
        alive.append(jnp.where(finished[c] == 0, 1, 0))

    position = lax.broadcasted_iota(jnp.int32, (slots, local), 0)
    for c in range(spans):
        length = cache_len[c]
        older = jnp.where(position < length * alive[c], 1.0, 0.0).astype(jnp.bfloat16)
        fresh = jnp.where(position == jnp.where(alive[c] == 1, length, -1), 1.0, 0.0).astype(
            jnp.bfloat16
        )
        for a in range(2):
            updated[a, c] = self_cache[a, c] * older + token_qkv[1 + a, c : c + 1, :] * fresh

    def flag(value, shape):
        return jnp.full(shape, jnp.where(value, 1.0, 0.0), jnp.float32).astype(jnp.bfloat16)

    marker_row = lax.broadcasted_iota(jnp.int32, mark.shape[1:], 0)
    for i, distance in enumerate(DISTANCES):
        marker = jnp.zeros(mark.shape[1:], jnp.float32)
        for c in range(spans):
            at = jnp.where(offset[c] == distance, place[c], -1)
            marker = jnp.where(marker_row == at, 1.0, marker)
        mark[i] = marker.astype(jnp.bfloat16)

    def send(source, target, sems, i, distance):
        return pltpu.make_async_remote_copy(
            src_ref=source,
            dst_ref=target,
            send_sem=sems.at[0, i],
            recv_sem=sems.at[1, i],
            device_id={"batch": targets[i]},
            device_id_type=MESH,
        )

    pl.semaphore_wait(barrier, len(targets) + len(others))
    mark_copies, cache_copies = [], []
    for i, distance in enumerate(DISTANCES):
        copy = send(mark.at[i], mark_in.at[i], mark_sems, i, distance)
        copy.start()
        mark_copies.append(copy)
    for i, distance in enumerate(DISTANCES):
        for a in range(2):
            total = updated[a, 0] * flag(offset[0] == distance, (1, local))
            for c in range(1, spans):
                total = total + updated[a, c] * flag(offset[c] == distance, (1, local))
            parcel[i, a] = total
        copy = send(parcel.at[i], arrived.at[i], cache_sems, i, distance)
        copy.start()
        cache_copies.append(copy)

    for l in range(spans):
        for a in range(2):
            total = updated[a, 0] * flag((offset[0] == 0) & (place[0] == l), (1, local))
            for c in range(1, spans):
                keep = flag((offset[c] == 0) & (place[c] == l), (1, local))
                total = total + updated[a, c] * keep
            moved_cache[a, l] = total

    contexts = []
    for c in range(spans):
        query, key, value = (token_qkv[k, c : c + 1, :] for k in range(3))
        contexts.append(
            attend(query, self_cache[0, c], self_cache[1, c], cache_len[c], (key, value))
        )
    pad = part.shape[0] - spans
    context = jnp.concatenate(contexts + [jnp.zeros((pad, local), jnp.float32)], 0)
    context = context.astype(jnp.bfloat16)
    loads[0].wait()
    part[...] = jnp.dot(context, out_proj[...], preferred_element_type=jnp.float32)
    part_copies = []
    for k, other in enumerate(others):
        copy = pltpu.make_async_remote_copy(
            src_ref=part,
            dst_ref=part_in.at[k],
            send_sem=part_sems.at[0, k],
            recv_sem=part_sems.at[1, k],
            device_id={"mp": other},
            device_id_type=MESH,
        )
        copy.start()
        part_copies.append(copy)
    loads[1].wait()
    loads[2].wait()
    for copy in part_copies:
        copy.wait()
    summed = part[...]
    for k in range(len(others)):
        summed = summed + part_in[k]
    resid = hidden[...].astype(jnp.float32) + summed[:spans]
    centre = jnp.mean(resid, axis=-1, keepdims=True)
    spread = jnp.mean((resid - centre) ** 2, axis=-1, keepdims=True)
    gain = ln_gain[...].reshape(1, width)
    bias = ln_bias[...].reshape(1, width)
    normed = (resid - centre) * lax.rsqrt(spread + 1e-05) * gain + bias
    normed = jnp.concatenate([normed, jnp.zeros((pad, width), jnp.float32)], 0)
    query = jnp.dot(
        normed.astype(jnp.bfloat16), query_proj[...], preferred_element_type=jnp.float32
    ).astype(jnp.bfloat16).astype(jnp.float32)
    decoded = []
    for c in range(spans):
        mixed = attend(query[c : c + 1], cross[0, c], cross[1, c], None, None)
        decoded.append(mixed * jnp.where(alive[c] == 1, 1.0, 0.0))

    line_copies = []
    blank = jnp.zeros((line.shape[1] - 1, local), jnp.float32)
    for i, distance in enumerate(DISTANCES):
        row = jnp.zeros((1, local), jnp.float32)
        for c in range(spans):
            row = row + decoded[c] * jnp.where(offset[c] == distance, 1.0, 0.0)
        line[i] = jnp.concatenate([row, blank], 0).astype(jnp.bfloat16)
        copy = send(line.at[i], line_in.at[i], line_sems, i, distance)
        copy.start()
        line_copies.append(copy)

    rows = []
    for l in range(spans):
        row = jnp.zeros((1, local), jnp.float32)
        for c in range(spans):
            keep = (offset[c] == 0) & (place[c] == l)
            row = row + decoded[c] * jnp.where(keep, 1.0, 0.0)
        rows.append(row)
    for i in range(len(DISTANCES)):
        mark_copies[i].wait()
        cache_copies[i].wait()
        for l in range(spans):
            taken = mark_in[i, l : l + 1, :]
            for a in range(2):
                moved_cache[a, l] = moved_cache[a, l] + arrived[i, a] * taken
    for i in range(len(DISTANCES)):
        line_copies[i].wait()
        for l in range(spans):
            taken = mark_in[i, l : l + 1, :].astype(jnp.float32)
            rows[l] = rows[l] + line_in[i, 0:1, :].astype(jnp.float32) * taken
    moved_out[...] = jnp.concatenate(rows, 0).astype(jnp.bfloat16)


def relay_kernel(
    count,
    cores,
    cache_len,
    finished,
    new_slot,
    hidden,
    token_qkv,
    cache_hbm,
    ln_gain,
    ln_bias,
    cross_hbm,
    out_proj_hbm,
    query_proj_hbm,
    moved_cache,
    moved_out,
    self_cache,
    cross,
    out_proj,
    query_proj,
    own,
    raw_in,
    cross_out,
    cross_in,
    kept,
    final_out,
    final_in,
    final_far,
    pick,
    label,
    label_in,
    line,
    line_in,
    line_kept,
    line_out,
    line_cross,
    line_last,
    line_final,
    part,
    part_in,
    load_sem,
    raw_send,
    raw_recv,
    hop_sems,
    label_send,
    label_recv,
    line_send,
    line_recv,
    line_hops,
    part_sems,
):
    spans, width = hidden.shape
    slots, local = self_cache.shape[2:]
    steps, _, rows_per, _ = own.shape
    per = steps // 2
    me = lax.axis_index("batch")
    core = lax.axis_index("mp")
    level, column = lax.div(me, 2), lax.rem(me, 2)
    inner = (level == 1) | (level == REACH - 1)
    outer = jnp.logical_not(inner)
    barrier = pltpu.get_barrier_semaphore()

    def greet(where):
        pl.semaphore_signal(barrier, inc=1, device_id=where, device_id_type=MESH)

    mate_level = jnp.where(level == 0, 1, jnp.where(level == 1, 0, jnp.where(level == 2, 3, 2)))
    mate = mate_level * 2 + column
    mate_aside = mate_level * 2 + 1 - column
    aside = level * 2 + 1 - column
    across = (REACH - level) * 2 + column
    beyond = (REACH - mate_level) * 2 + column
    others = [lax.rem(core + k, cores) for k in range(1, cores)]
    for node in (mate, mate_aside, beyond):
        greet({"batch": node})

    @pl.when(inner)
    def _():
        greet({"batch": aside})
        greet({"batch": across})

    for other in others:
        greet({"mp": other})
    loads = [
        pltpu.make_async_copy(source, target, load_sem.at[i])
        for i, (source, target) in enumerate(
            [
                (out_proj_hbm, out_proj),
                (query_proj_hbm, query_proj),
                (cross_hbm, cross),
                (cache_hbm.at[0], self_cache.at[0]),
                (cache_hbm.at[1], self_cache.at[1]),
            ]
        )
    ]
    for i in (3, 4, 0, 1, 2):
        loads[i].start()

    alive = [jnp.where(finished[c] == 0, 1, 0) for c in range(spans)]

    def to(node, source, target, sent, received):
        return pltpu.make_async_remote_copy(
            src_ref=source,
            dst_ref=target,
            send_sem=sent,
            recv_sem=received,
            device_id={"batch": node},
            device_id_type=MESH,
        )

    def raw_copy(node, lane, way, k):
        return to(node, own.at[k], raw_in.at[way, k], raw_send.at[lane, k], raw_recv.at[way, k])

    def far_copy(k):
        return to(
            beyond,
            cross_out.at[k, pl.ds(spans, spans)],
            final_far.at[k],
            hop_sems.at[0, k],
            hop_sems.at[1, k],
        )

    def cross_copy(k):
        return to(
            across,
            cross_out.at[k, pl.ds(0, spans)],
            cross_in.at[k],
            hop_sems.at[2, k],
            hop_sems.at[3, k],
        )

    def final_copy(k):
        return to(mate, final_out.at[k], final_in.at[k], hop_sems.at[4, k], hop_sems.at[5, k])

    def label_copy(node, lane, way):
        return to(node, label, label_in.at[way], label_send.at[lane], label_recv.at[way])

    def line_copy(node, lane, way):
        return to(node, line, line_in.at[way], line_send.at[lane], line_recv.at[way])

    def line_cross_copy():
        return to(across, line_out, line_cross, line_hops.at[0], line_hops.at[1])

    def line_final_copy():
        return to(mate, line_last, line_final, line_hops.at[2], line_hops.at[3])

    label_row = lax.broadcasted_iota(jnp.int32, label.shape, 0)
    labels = jnp.zeros(label.shape, jnp.int32)
    for c in range(spans):
        labels = jnp.where(label_row == c, new_slot[c], labels)
    label[...] = labels.astype(jnp.float32)

    @pl.when(inner)
    def _():
        pl.semaphore_wait(barrier, 5 + len(others))

    @pl.when(outer)
    def _():
        pl.semaphore_wait(barrier, 3 + len(others))

    position = lax.broadcasted_iota(jnp.int32, (rows_per, local), 0)
    ends = [cache_len[c] * alive[c] for c in range(spans)]
    fresh_at = [jnp.where(alive[c] == 1, cache_len[c], -1) for c in range(spans)]

    def grow(k, _):
        a, r = lax.div(k, per), lax.rem(k, per)
        start = pl.multiple_of(r * rows_per, rows_per)
        at = position + start
        for c in range(spans):
            older = jnp.where(at < ends[c], 1.0, 0.0).astype(jnp.bfloat16)
            fresh = jnp.where(at == fresh_at[c], 1.0, 0.0).astype(jnp.bfloat16)
            new = jnp.where(a == 0, token_qkv[1, c : c + 1, :].astype(jnp.float32),
                            token_qkv[2, c : c + 1, :].astype(jnp.float32)).astype(jnp.bfloat16)
            own[k, c] = self_cache[a, c, pl.ds(start, rows_per), :] * older + new * fresh

        return 0

    def pass_on(k, _):
        @pl.when(outer)
        def _():
            raw_copy(mate, 0, 0, k).start()
            raw_copy(mate_aside, 1, 1, k).start()

        @pl.when(inner)
        def _():
            raw_copy(aside, 0, 2, k).start()

        return 0

    def grow_and_pass(k, _):
        grow(k, 0)
        pass_on(k, 0)
        return 0

    @pl.when(outer)
    def _():
        label_copy(mate, 0, 0).start()
        label_copy(mate_aside, 1, 1).start()

    @pl.when(inner)
    def _():
        label_copy(aside, 0, 2).start()

    loads[3].wait()
    lax.fori_loop(0, per, grow_and_pass, 0)
    loads[4].wait()
    lax.fori_loop(per, HOLD, grow_and_pass, 0)
    lax.fori_loop(HOLD, steps, grow, 0)

    def self_part():
        contexts = []
        for c in range(spans):
            query, key, value = (token_qkv[k, c : c + 1, :] for k in range(3))
            contexts.append(
                attend(query, self_cache[0, c], self_cache[1, c], cache_len[c], (key, value))
            )
        context = jnp.concatenate(contexts + [jnp.zeros((pad, local), jnp.float32)], 0)
        context = context.astype(jnp.bfloat16)
        loads[0].wait()
        part[...] = jnp.dot(context, out_proj[...], preferred_element_type=jnp.float32)

    def part_copy(k):
        return pltpu.make_async_remote_copy(
            src_ref=part,
            dst_ref=part_in.at[k],
            send_sem=part_sems.at[0, k],
            recv_sem=part_sems.at[1, k],
            device_id={"mp": others[k]},
            device_id_type=MESH,
        )

    pad = part.shape[0] - spans
    self_part()
    for k in range(len(others)):
        part_copy(k).start()

    @pl.when(inner)
    def _():
        for way in range(3):
            label_copy(mate, 0, way).wait_recv()
        sources = [label] + [label_in.at[way] for way in range(3)]
        nodes = [me, mate, across, beyond]
        for s, source in enumerate(sources):
            for c in range(spans):
                held = jnp.broadcast_to(source[c : c + 1, 0:1], (rows_per, local))
                for d, node in enumerate(nodes):
                    for l in range(spans):
                        wanted = jnp.full((rows_per, local), node * spans + l, jnp.int32)
                        pick[s * spans + c, d * spans + l] = jnp.where(
                            held == wanted.astype(jnp.float32), 1.0, 0.0
                        ).astype(jnp.bfloat16)

    def merge(k, _):
        for way in range(3):
            raw_copy(mate, 0, way, k).wait_recv()
        blocks = [own[k, c] for c in range(spans)]
        for way in range(3):
            blocks += [raw_in[way, k, c] for c in range(spans)]

        def gathered(d):
            total = blocks[0] * pick[0, d]
            for s in range(1, len(blocks)):
                total = total + blocks[s] * pick[s, d]
            return total

        for d in range(spans, 2 * spans):
            cross_out[k, d] = gathered(2 * spans + d)
        far_copy(k).start()
        for d in range(spans):
            cross_out[k, d] = gathered(2 * spans + d)
        cross_copy(k).start()
        for d in range(spans):
            final_out[k, d] = gathered(spans + d)
        final_copy(k).start()
        for d in range(spans):
            kept[k, d] = gathered(d)
        return 0

    def finish(k, _):
        cross_copy(k).wait_recv()
        a, r = lax.div(k, per), lax.rem(k, per)
        start = pl.multiple_of(r * rows_per, rows_per)
        for l in range(spans):
            moved_cache[a, l, pl.ds(start, rows_per), :] = kept[k, l] + cross_in[k, l]
        return 0

    def both(k, _):
        merge(k, 0)
        finish(k - LAG, 0)
        return 0

    @pl.when(inner)
    def _():
        lax.fori_loop(0, EARLY, merge, 0)

    loads[1].wait()
    loads[2].wait()
    for k in range(len(others)):
        part_copy(k).wait()
    summed = part[...]
    for k in range(len(others)):
        summed = summed + part_in[k]
    resid = hidden[...].astype(jnp.float32) + summed[:spans]
    centre = jnp.mean(resid, axis=-1, keepdims=True)
    spread = jnp.mean((resid - centre) ** 2, axis=-1, keepdims=True)
    gain = ln_gain[...].reshape(1, width)
    bias = ln_bias[...].reshape(1, width)
    normed = (resid - centre) * lax.rsqrt(spread + 1e-05) * gain + bias
    normed = jnp.concatenate([normed, jnp.zeros((pad, width), jnp.float32)], 0)
    query = jnp.dot(
        normed.astype(jnp.bfloat16), query_proj[...], preferred_element_type=jnp.float32
    ).astype(jnp.bfloat16).astype(jnp.float32)

    @pl.when(inner)
    def _():
        lax.fori_loop(EARLY, LAG, merge, 0)

    decoded = []
    for c in range(spans):
        mixed = attend(query[c : c + 1], cross[0, c], cross[1, c], None, None)
        decoded.append(mixed * jnp.where(alive[c] == 1, 1.0, 0.0))

    line[...] = jnp.concatenate(decoded, 0).astype(jnp.bfloat16)

    @pl.when(outer)
    def _():
        line_copy(mate, 0, 0).start()
        line_copy(mate_aside, 1, 1).start()

    @pl.when(inner)
    def _():
        line_copy(aside, 0, 2).start()

    lax.fori_loop(HOLD, steps, pass_on, 0)

    @pl.when(inner)
    def _():
        lax.fori_loop(LAG, MIDDLE, both, 0)
        for way in range(3):
            line_copy(mate, 0, way).wait_recv()
        blocks = []
        for held in [line] + [line_in.at[way] for way in range(3)]:
            blocks += [held[c : c + 1, :].astype(jnp.float32) for c in range(spans)]
        rows = []
        for d in range(4 * spans):
            total = blocks[0] * pick[0, d, 0:1, :].astype(jnp.float32)
            for s in range(1, len(blocks)):
                total = total + blocks[s] * pick[s, d, 0:1, :].astype(jnp.float32)
            rows.append(total)
        line_out[...] = jnp.concatenate(rows[2 * spans :], 0).astype(jnp.bfloat16)
        line_cross_copy().start()
        line_kept[...] = jnp.concatenate(rows[: 2 * spans], 0)
        lax.fori_loop(MIDDLE, steps, both, 0)
        line_cross_copy().wait_recv()
        total = line_kept[...] + line_cross[...].astype(jnp.float32)
        line_last[...] = total[spans:].astype(jnp.bfloat16)
        line_final_copy().start()
        moved_out[...] = total[:spans].astype(jnp.bfloat16)

    def land(k, _):
        final_copy(k).wait_recv()
        far_copy(k).wait_recv()
        a, r = lax.div(k, per), lax.rem(k, per)
        start = pl.multiple_of(r * rows_per, rows_per)
        for l in range(spans):
            moved_cache[a, l, pl.ds(start, rows_per), :] = final_in[k, l] + final_far[k, l]
        return 0

    def outer_sent(k, _):
        raw_copy(mate, 0, 0, k).wait_send()
        raw_copy(mate_aside, 1, 1, k).wait_send()
        return 0

    def inner_sent(k, _):
        raw_copy(aside, 0, 2, k).wait_send()
        far_copy(k).wait_send()
        cross_copy(k).wait_send()
        final_copy(k).wait_send()
        return 0

    @pl.when(inner)
    def _():
        lax.fori_loop(steps - LAG, steps, finish, 0)
        label_copy(aside, 0, 2).wait_send()
        line_copy(aside, 0, 2).wait_send()
        line_cross_copy().wait_send()
        line_final_copy().wait_send()
        lax.fori_loop(0, steps, inner_sent, 0)

    @pl.when(outer)
    def _():
        lax.fori_loop(0, steps, land, 0)
        label_copy(mate, 0, 0).wait_send()
        label_copy(mate_aside, 1, 1).wait_send()
        line_copy(mate, 0, 0).wait_send()
        line_copy(mate_aside, 1, 1).wait_send()
        line_final_copy().wait_recv()
        moved_out[...] = line_final[...]
        lax.fori_loop(0, steps, outer_sent, 0)


def body(
    hidden,
    token_qkv,
    self_cache,
    cross_kv,
    cache_len,
    finished,
    new_slot,
    out_proj,
    ln_gain,
    ln_bias,
    query_proj,
):
    count, cores = lax.axis_size("batch"), lax.axis_size("mp")
    spans, width = hidden.shape
    slots, local = self_cache.shape[2:]
    moves = len(DISTANCES)
    smem = pl.BlockSpec(memory_space=pltpu.SMEM)
    vmem = pl.BlockSpec(memory_space=pltpu.VMEM)
    away = pl.BlockSpec(memory_space=pl.ANY)
    bf16, f32 = jnp.bfloat16, jnp.float32
    operands = (
        cache_len,
        finished,
        new_slot,
        hidden,
        token_qkv,
        self_cache,
        ln_gain,
        ln_bias,
        cross_kv,
        out_proj,
        query_proj,
    )
    parcels = pltpu.VMEM((moves, 2, slots, local), bf16)
    tiles = pltpu.VMEM((moves, 16, local), bf16)
    dma = pltpu.SemaphoreType.DMA
    inputs = [pltpu.VMEM(array.shape, bf16) for array in (cross_kv, out_proj, query_proj)]
    parts = [pltpu.VMEM((8, width), f32), pltpu.VMEM((cores - 1, 8, width), f32)]
    steps = 2 * slots // ROWS
    if count == 2 * (REACH + 1):
        function, cache_spec = relay_kernel, away

        def blocks(*lead):
            return pltpu.VMEM(lead + (ROWS, local), bf16)

        scratch = [pltpu.VMEM(self_cache.shape, bf16)] + inputs + [
            blocks(steps, spans),
            blocks(3, steps, spans),
            blocks(steps, 2 * spans),
            blocks(steps, spans),
            blocks(steps, spans),
            blocks(steps, spans),
            blocks(steps, spans),
            blocks(steps, spans),
            blocks(4 * spans, 4 * spans),
            pltpu.VMEM((8, 128), f32),
            pltpu.VMEM((3, 8, 128), f32),
            pltpu.VMEM((spans, local), bf16),
            pltpu.VMEM((3, spans, local), bf16),
            pltpu.VMEM((2 * spans, local), f32),
            pltpu.VMEM((2 * spans, local), bf16),
            pltpu.VMEM((2 * spans, local), bf16),
            pltpu.VMEM((spans, local), bf16),
            pltpu.VMEM((spans, local), bf16),
            *parts,
            dma((5,)),
            dma((2, steps)),
            dma((3, steps)),
            dma((6, steps)),
            dma((2,)),
            dma((3,)),
            dma((2,)),
            dma((3,)),
            dma((4,)),
            dma((2, cores - 1)),
        ]
    else:
        function, cache_spec = kernel, vmem
        scratch = inputs + [
            pltpu.VMEM(self_cache.shape, bf16),
            parcels,
            parcels,
            tiles,
            tiles,
            tiles,
            tiles,
            *parts,
            dma((3,)),
            dma((2, moves)),
            dma((2, moves)),
            dma((2, moves)),
            dma((2, cores - 1)),
        ]
    return pl.pallas_call(
        functools.partial(function, count, cores),
        out_shape=(
            pltpu.VMEM(self_cache.shape, bf16),
            pltpu.VMEM((spans, local), bf16),
        ),
        in_specs=[smem] * 3 + [vmem] * 2 + [cache_spec] + [vmem] * 2 + [away] * 3,
        out_specs=(vmem, vmem),
        scratch_shapes=scratch,
        compiler_params=pltpu.CompilerParams(collective_id=0, has_side_effects=True),
    )(*operands)


def solution(mesh):
    placed = (
        P(("groups", "batch"), None),
        P(None, ("groups", "batch"), "mp"),
        P(None, ("groups", "batch"), None, "mp"),
        P(None, ("groups", "batch"), None, "mp"),
        P(("groups", "batch")),
        P(("groups", "batch")),
        P(("groups", "batch")),
        P("mp", None),
        P(),
        P(),
        P(None, "mp"),
    )
    return jax.shard_map(
        body,
        mesh=mesh,
        in_specs=placed,
        out_specs=(P(None, ("groups", "batch"), None, "mp"), P(("groups", "batch"), "mp")),
        check_vma=False,
    )
```

```python
import functools

import jax
import jax.numpy as jnp
from jax import lax
from jax.experimental import pallas as pl
from jax.experimental.pallas import tpu as pltpu
from jax.sharding import PartitionSpec as P

HEAD_DIM = 64
REACH = 3
MESH = pl.DeviceIdType.MESH
DISTANCES = [3, -3, 2, -2, 1, -1]
ROWS = 16
LAG = 3
EARLY = 1
MIDDLE = 14
HOLD = 8


def attend(query, keys, values, length, own):
    slots, width = keys.shape
    heads = width // HEAD_DIM
    rows = -(-heads // 16) * 16
    row = lax.broadcasted_iota(jnp.int32, (rows, width), 0)
    column = lax.broadcasted_iota(jnp.int32, (rows, width), 1)
    low = row * HEAD_DIM
    mine = (column >= low) & (column < low + HEAD_DIM)
    spread = jnp.where(mine, query.astype(jnp.float32), 0.0)
    factor = HEAD_DIM ** (-0.5)
    scores = (
        lax.dot_general(
            spread.astype(jnp.bfloat16),
            keys,
            (((1,), (1,)), ((), ())),
            preferred_element_type=jnp.float32,
        )
        * factor
    )
    if length is not None:
        usable = lax.broadcasted_iota(jnp.int32, (rows, slots), 1) < length
        scores = jnp.where(usable, scores, -1e30)
    highest = jnp.max(scores, axis=-1, keepdims=True)
    if own is not None:
        new_key, new_value = own
        own_score = jnp.sum(spread * new_key.astype(jnp.float32), axis=-1, keepdims=True) * factor
        highest = jnp.maximum(highest, own_score)
    weight = jnp.exp(scores - highest)
    if length is not None:
        weight = jnp.where(usable, weight, 0.0)
    total = jnp.sum(weight, axis=-1, keepdims=True)
    if own is not None:
        own_weight = jnp.exp(own_score - highest)
        total = total + own_weight
    weight = (weight / total).astype(jnp.bfloat16)
    mixed = jnp.dot(weight, values, preferred_element_type=jnp.float32)
    if own is not None:
        own_weight = (own_weight / total).astype(jnp.bfloat16).astype(jnp.float32)
        mixed = mixed + own_weight * new_value.astype(jnp.float32)
    return jnp.sum(jnp.where(mine, mixed, 0.0), axis=0, keepdims=True)


def kernel(
    count,
    cores,
    cache_len,
    finished,
    new_slot,
    hidden,
    token_qkv,
    self_cache,
    ln_gain,
    ln_bias,
    cross_hbm,
    out_proj_hbm,
    query_proj_hbm,
    moved_cache,
    moved_out,
    cross,
    out_proj,
    query_proj,
    updated,
    parcel,
    arrived,
    mark,
    mark_in,
    line,
    line_in,
    part,
    part_in,
    load_sem,
    cache_sems,
    mark_sems,
    line_sems,
    part_sems,
):
    spans, width = hidden.shape
    slots, local = self_cache.shape[2:]
    me = lax.axis_index("batch")
    core = lax.axis_index("mp")
    loads = [
        pltpu.make_async_copy(source, target, load_sem.at[i])
        for i, (source, target) in enumerate(
            [(out_proj_hbm, out_proj), (query_proj_hbm, query_proj), (cross_hbm, cross)]
        )
    ]
    for load in loads:
        load.start()

    barrier = pltpu.get_barrier_semaphore()
    targets = [lax.rem(me + distance + count, count) for distance in DISTANCES]
    for target in targets:
        pl.semaphore_signal(barrier, inc=1, device_id={"batch": target}, device_id_type=MESH)
    others = [lax.rem(core + k, cores) for k in range(1, cores)]
    for other in others:
        pl.semaphore_signal(barrier, inc=1, device_id={"mp": other}, device_id_type=MESH)

    half = count // 2
    alive, offset, place = [], [], []
    for c in range(spans):
        slot = new_slot[c]
        owner = lax.div(slot, spans)
        offset.append(lax.rem(owner - me + half + count, count) - half)
        place.append(lax.rem(slot, spans))
        alive.append(jnp.where(finished[c] == 0, 1, 0))

    position = lax.broadcasted_iota(jnp.int32, (slots, local), 0)
    for c in range(spans):
        length = cache_len[c]
        older = jnp.where(position < length * alive[c], 1.0, 0.0).astype(jnp.bfloat16)
        fresh = jnp.where(position == jnp.where(alive[c] == 1, length, -1), 1.0, 0.0).astype(
            jnp.bfloat16
        )
        for a in range(2):
            updated[a, c] = self_cache[a, c] * older + token_qkv[1 + a, c : c + 1, :] * fresh

    def flag(value, shape):
        return jnp.full(shape, jnp.where(value, 1.0, 0.0), jnp.float32).astype(jnp.bfloat16)

    marker_row = lax.broadcasted_iota(jnp.int32, mark.shape[1:], 0)
    for i, distance in enumerate(DISTANCES):
        marker = jnp.zeros(mark.shape[1:], jnp.float32)
        for c in range(spans):
            at = jnp.where(offset[c] == distance, place[c], -1)
            marker = jnp.where(marker_row == at, 1.0, marker)
        mark[i] = marker.astype(jnp.bfloat16)

    def send(source, target, sems, i, distance):
        return pltpu.make_async_remote_copy(
            src_ref=source,
            dst_ref=target,
            send_sem=sems.at[0, i],
            recv_sem=sems.at[1, i],
            device_id={"batch": targets[i]},
            device_id_type=MESH,
        )

    pl.semaphore_wait(barrier, len(targets) + len(others))
    mark_copies, cache_copies = [], []
    for i, distance in enumerate(DISTANCES):
        copy = send(mark.at[i], mark_in.at[i], mark_sems, i, distance)
        copy.start()
        mark_copies.append(copy)
    for i, distance in enumerate(DISTANCES):
        for a in range(2):
            total = updated[a, 0] * flag(offset[0] == distance, (1, local))
            for c in range(1, spans):
                total = total + updated[a, c] * flag(offset[c] == distance, (1, local))
            parcel[i, a] = total
        copy = send(parcel.at[i], arrived.at[i], cache_sems, i, distance)
        copy.start()
        cache_copies.append(copy)

    for l in range(spans):
        for a in range(2):
            total = updated[a, 0] * flag((offset[0] == 0) & (place[0] == l), (1, local))
            for c in range(1, spans):
                keep = flag((offset[c] == 0) & (place[c] == l), (1, local))
                total = total + updated[a, c] * keep
            moved_cache[a, l] = total

    contexts = []
    for c in range(spans):
        query, key, value = (token_qkv[k, c : c + 1, :] for k in range(3))
        contexts.append(
            attend(query, self_cache[0, c], self_cache[1, c], cache_len[c], (key, value))
        )
    pad = part.shape[0] - spans
    context = jnp.concatenate(contexts + [jnp.zeros((pad, local), jnp.float32)], 0)
    context = context.astype(jnp.bfloat16)
    loads[0].wait()
    part[...] = jnp.dot(context, out_proj[...], preferred_element_type=jnp.float32)
    part_copies = []
    for k, other in enumerate(others):
        copy = pltpu.make_async_remote_copy(
            src_ref=part,
            dst_ref=part_in.at[k],
            send_sem=part_sems.at[0, k],
            recv_sem=part_sems.at[1, k],
            device_id={"mp": other},
            device_id_type=MESH,
        )
        copy.start()
        part_copies.append(copy)
    loads[1].wait()
    loads[2].wait()
    for copy in part_copies:
        copy.wait()
    summed = part[...]
    for k in range(len(others)):
        summed = summed + part_in[k]
    resid = hidden[...].astype(jnp.float32) + summed[:spans]
    centre = jnp.mean(resid, axis=-1, keepdims=True)
    spread = jnp.mean((resid - centre) ** 2, axis=-1, keepdims=True)
    gain = ln_gain[...].reshape(1, width)
    bias = ln_bias[...].reshape(1, width)
    normed = (resid - centre) * lax.rsqrt(spread + 1e-05) * gain + bias
    normed = jnp.concatenate([normed, jnp.zeros((pad, width), jnp.float32)], 0)
    query = jnp.dot(
        normed.astype(jnp.bfloat16), query_proj[...], preferred_element_type=jnp.float32
    ).astype(jnp.bfloat16).astype(jnp.float32)
    decoded = []
    for c in range(spans):
        mixed = attend(query[c : c + 1], cross[0, c], cross[1, c], None, None)
        decoded.append(mixed * jnp.where(alive[c] == 1, 1.0, 0.0))

    line_copies = []
    blank = jnp.zeros((line.shape[1] - 1, local), jnp.float32)
    for i, distance in enumerate(DISTANCES):
        row = jnp.zeros((1, local), jnp.float32)
        for c in range(spans):
            row = row + decoded[c] * jnp.where(offset[c] == distance, 1.0, 0.0)
        line[i] = jnp.concatenate([row, blank], 0).astype(jnp.bfloat16)
        copy = send(line.at[i], line_in.at[i], line_sems, i, distance)
        copy.start()
        line_copies.append(copy)

    rows = []
    for l in range(spans):
        row = jnp.zeros((1, local), jnp.float32)
        for c in range(spans):
            keep = (offset[c] == 0) & (place[c] == l)
            row = row + decoded[c] * jnp.where(keep, 1.0, 0.0)
        rows.append(row)
    for i in range(len(DISTANCES)):
        mark_copies[i].wait()
        cache_copies[i].wait()
        for l in range(spans):
            taken = mark_in[i, l : l + 1, :]
            for a in range(2):
                moved_cache[a, l] = moved_cache[a, l] + arrived[i, a] * taken
    for i in range(len(DISTANCES)):
        line_copies[i].wait()
        for l in range(spans):
            taken = mark_in[i, l : l + 1, :].astype(jnp.float32)
            rows[l] = rows[l] + line_in[i, 0:1, :].astype(jnp.float32) * taken
    moved_out[...] = jnp.concatenate(rows, 0).astype(jnp.bfloat16)


def relay_kernel(
    count,
    cores,
    cache_len_hbm,
    finished_hbm,
    new_slot_hbm,
    hidden_hbm,
    token_qkv_hbm,
    cache_hbm,
    ln_gain_hbm,
    ln_bias_hbm,
    cross_hbm,
    out_proj_hbm,
    query_proj_hbm,
    moved_cache,
    moved_out,
    cache_len,
    finished,
    new_slot,
    hidden,
    token_qkv,
    ln_gain,
    ln_bias,
    self_cache,
    cross,
    out_proj,
    query_proj,
    own,
    raw_in,
    cross_out,
    cross_in,
    kept,
    final_out,
    final_in,
    final_far,
    pick,
    label,
    label_in,
    line,
    line_in,
    line_kept,
    line_out,
    line_cross,
    line_last,
    line_final,
    part,
    part_in,
    load_sem,
    raw_send,
    raw_recv,
    hop_sems,
    label_send,
    label_recv,
    line_send,
    line_recv,
    line_hops,
    part_sems,
):
    spans, width = hidden.shape
    slots, local = self_cache.shape[2:]
    steps, _, rows_per, _ = own.shape
    per = steps // 2
    me = lax.axis_index("batch")
    core = lax.axis_index("mp")
    level, column = lax.div(me, 2), lax.rem(me, 2)
    inner = (level == 1) | (level == REACH - 1)
    outer = jnp.logical_not(inner)
    barrier = pltpu.get_barrier_semaphore()

    def greet(where):
        pl.semaphore_signal(barrier, inc=1, device_id=where, device_id_type=MESH)

    mate_level = jnp.where(level == 0, 1, jnp.where(level == 1, 0, jnp.where(level == 2, 3, 2)))
    mate = mate_level * 2 + column
    mate_aside = mate_level * 2 + 1 - column
    aside = level * 2 + 1 - column
    across = (REACH - level) * 2 + column
    beyond = (REACH - mate_level) * 2 + column
    others = [lax.rem(core + k, cores) for k in range(1, cores)]
    for node in (mate, mate_aside, beyond):
        greet({"batch": node})

    @pl.when(inner)
    def _():
        greet({"batch": aside})
        greet({"batch": across})

    for other in others:
        greet({"mp": other})
    loads = [
        pltpu.make_async_copy(source, target, load_sem.at[i])
        for i, (source, target) in enumerate(
            [
                (out_proj_hbm, out_proj),
                (query_proj_hbm, query_proj),
                (cross_hbm, cross),
                (cache_hbm.at[0], self_cache.at[0]),
                (cache_hbm.at[1], self_cache.at[1]),
                (cache_len_hbm, cache_len),
                (finished_hbm, finished),
                (new_slot_hbm, new_slot),
                (hidden_hbm, hidden),
                (token_qkv_hbm, token_qkv),
                (ln_gain_hbm, ln_gain),
                (ln_bias_hbm, ln_bias),
            ]
        )
    ]
    for i in [3, *range(5, len(loads)), 4, 0, 1, 2]:
        loads[i].start()
    for load in loads[5:]:
        load.wait()

    alive = [jnp.where(finished[c] == 0, 1, 0) for c in range(spans)]

    def to(node, source, target, sent, received):
        return pltpu.make_async_remote_copy(
            src_ref=source,
            dst_ref=target,
            send_sem=sent,
            recv_sem=received,
            device_id={"batch": node},
            device_id_type=MESH,
        )

    def raw_copy(node, lane, way, k):
        return to(node, own.at[k], raw_in.at[way, k], raw_send.at[lane, k], raw_recv.at[way, k])

    def far_copy(k):
        return to(
            beyond,
            cross_out.at[k, pl.ds(spans, spans)],
            final_far.at[k],
            hop_sems.at[0, k],
            hop_sems.at[1, k],
        )

    def cross_copy(k):
        return to(
            across,
            cross_out.at[k, pl.ds(0, spans)],
            cross_in.at[k],
            hop_sems.at[2, k],
            hop_sems.at[3, k],
        )

    def final_copy(k):
        return to(mate, final_out.at[k], final_in.at[k], hop_sems.at[4, k], hop_sems.at[5, k])

    def label_copy(node, lane, way):
        return to(node, label, label_in.at[way], label_send.at[lane], label_recv.at[way])

    def line_copy(node, lane, way):
        return to(node, line, line_in.at[way], line_send.at[lane], line_recv.at[way])

    def line_cross_copy():
        return to(across, line_out, line_cross, line_hops.at[0], line_hops.at[1])

    def line_final_copy():
        return to(mate, line_last, line_final, line_hops.at[2], line_hops.at[3])

    label_row = lax.broadcasted_iota(jnp.int32, label.shape, 0)
    labels = jnp.zeros(label.shape, jnp.int32)
    for c in range(spans):
        labels = jnp.where(label_row == c, new_slot[c], labels)
    label[...] = labels.astype(jnp.float32)

    @pl.when(inner)
    def _():
        pl.semaphore_wait(barrier, 5 + len(others))

    @pl.when(outer)
    def _():
        pl.semaphore_wait(barrier, 3 + len(others))

    position = lax.broadcasted_iota(jnp.int32, (rows_per, local), 0)
    ends = [cache_len[c] * alive[c] for c in range(spans)]
    fresh_at = [jnp.where(alive[c] == 1, cache_len[c], -1) for c in range(spans)]

    def grow(k, _):
        a, r = lax.div(k, per), lax.rem(k, per)
        start = pl.multiple_of(r * rows_per, rows_per)
        at = position + start
        for c in range(spans):
            older = jnp.where(at < ends[c], 1.0, 0.0).astype(jnp.bfloat16)
            fresh = jnp.where(at == fresh_at[c], 1.0, 0.0).astype(jnp.bfloat16)
            new = jnp.where(a == 0, token_qkv[1, c : c + 1, :].astype(jnp.float32),
                            token_qkv[2, c : c + 1, :].astype(jnp.float32)).astype(jnp.bfloat16)
            own[k, c] = self_cache[a, c, pl.ds(start, rows_per), :] * older + new * fresh

        return 0

    def pass_on(k, _):
        @pl.when(outer)
        def _():
            raw_copy(mate, 0, 0, k).start()
            raw_copy(mate_aside, 1, 1, k).start()

        @pl.when(inner)
        def _():
            raw_copy(aside, 0, 2, k).start()

        return 0

    def grow_and_pass(k, _):
        grow(k, 0)
        pass_on(k, 0)
        return 0

    @pl.when(outer)
    def _():
        label_copy(mate, 0, 0).start()
        label_copy(mate_aside, 1, 1).start()

    @pl.when(inner)
    def _():
        label_copy(aside, 0, 2).start()

    loads[3].wait()
    lax.fori_loop(0, per, grow_and_pass, 0)
    loads[4].wait()
    lax.fori_loop(per, HOLD, grow_and_pass, 0)
    lax.fori_loop(HOLD, steps, grow, 0)

    def self_part():
        contexts = []
        for c in range(spans):
            query, key, value = (token_qkv[k, c : c + 1, :] for k in range(3))
            contexts.append(
                attend(query, self_cache[0, c], self_cache[1, c], cache_len[c], (key, value))
            )
        context = jnp.concatenate(contexts + [jnp.zeros((pad, local), jnp.float32)], 0)
        context = context.astype(jnp.bfloat16)
        loads[0].wait()
        part[...] = jnp.dot(context, out_proj[...], preferred_element_type=jnp.float32)

    def part_copy(k):
        return pltpu.make_async_remote_copy(
            src_ref=part,
            dst_ref=part_in.at[k],
            send_sem=part_sems.at[0, k],
            recv_sem=part_sems.at[1, k],
            device_id={"mp": others[k]},
            device_id_type=MESH,
        )

    pad = part.shape[0] - spans
    self_part()
    for k in range(len(others)):
        part_copy(k).start()

    @pl.when(inner)
    def _():
        for way in range(3):
            label_copy(mate, 0, way).wait_recv()
        sources = [label] + [label_in.at[way] for way in range(3)]
        nodes = [me, mate, across, beyond]
        for s, source in enumerate(sources):
            for c in range(spans):
                held = jnp.broadcast_to(source[c : c + 1, 0:1], (rows_per, local))
                for d, node in enumerate(nodes):
                    for l in range(spans):
                        wanted = jnp.full((rows_per, local), node * spans + l, jnp.int32)
                        pick[s * spans + c, d * spans + l] = jnp.where(
                            held == wanted.astype(jnp.float32), 1.0, 0.0
                        ).astype(jnp.bfloat16)

    def merge(k, _):
        for way in range(3):
            raw_copy(mate, 0, way, k).wait_recv()
        blocks = [own[k, c] for c in range(spans)]
        for way in range(3):
            blocks += [raw_in[way, k, c] for c in range(spans)]

        def gathered(d):
            total = blocks[0] * pick[0, d]
            for s in range(1, len(blocks)):
                total = total + blocks[s] * pick[s, d]
            return total

        for d in range(spans, 2 * spans):
            cross_out[k, d] = gathered(2 * spans + d)
        far_copy(k).start()
        for d in range(spans):
            cross_out[k, d] = gathered(2 * spans + d)
        cross_copy(k).start()
        for d in range(spans):
            final_out[k, d] = gathered(spans + d)
        final_copy(k).start()
        for d in range(spans):
            kept[k, d] = gathered(d)
        return 0

    def finish(k, _):
        cross_copy(k).wait_recv()
        a, r = lax.div(k, per), lax.rem(k, per)
        start = pl.multiple_of(r * rows_per, rows_per)
        for l in range(spans):
            moved_cache[a, l, pl.ds(start, rows_per), :] = kept[k, l] + cross_in[k, l]
        return 0

    def both(k, _):
        merge(k, 0)
        finish(k - LAG, 0)
        return 0

    @pl.when(inner)
    def _():
        lax.fori_loop(0, EARLY, merge, 0)

    loads[1].wait()
    loads[2].wait()
    for k in range(len(others)):
        part_copy(k).wait()
    summed = part[...]
    for k in range(len(others)):
        summed = summed + part_in[k]
    resid = hidden[...].astype(jnp.float32) + summed[:spans]
    centre = jnp.mean(resid, axis=-1, keepdims=True)
    spread = jnp.mean((resid - centre) ** 2, axis=-1, keepdims=True)
    gain = ln_gain[...].reshape(1, width)
    bias = ln_bias[...].reshape(1, width)
    normed = (resid - centre) * lax.rsqrt(spread + 1e-05) * gain + bias
    normed = jnp.concatenate([normed, jnp.zeros((pad, width), jnp.float32)], 0)
    query = jnp.dot(
        normed.astype(jnp.bfloat16), query_proj[...], preferred_element_type=jnp.float32
    ).astype(jnp.bfloat16).astype(jnp.float32)

    @pl.when(inner)
    def _():
        lax.fori_loop(EARLY, LAG, merge, 0)

    decoded = []
    for c in range(spans):
        mixed = attend(query[c : c + 1], cross[0, c], cross[1, c], None, None)
        decoded.append(mixed * jnp.where(alive[c] == 1, 1.0, 0.0))

    line[...] = jnp.concatenate(decoded, 0).astype(jnp.bfloat16)

    @pl.when(outer)
    def _():
        line_copy(mate, 0, 0).start()
        line_copy(mate_aside, 1, 1).start()

    @pl.when(inner)
    def _():
        line_copy(aside, 0, 2).start()

    lax.fori_loop(HOLD, steps, pass_on, 0)

    @pl.when(inner)
    def _():
        lax.fori_loop(LAG, MIDDLE, both, 0)
        for way in range(3):
            line_copy(mate, 0, way).wait_recv()
        blocks = []
        for held in [line] + [line_in.at[way] for way in range(3)]:
            blocks += [held[c : c + 1, :].astype(jnp.float32) for c in range(spans)]
        rows = []
        for d in range(4 * spans):
            total = blocks[0] * pick[0, d, 0:1, :].astype(jnp.float32)
            for s in range(1, len(blocks)):
                total = total + blocks[s] * pick[s, d, 0:1, :].astype(jnp.float32)
            rows.append(total)
        line_out[...] = jnp.concatenate(rows[2 * spans :], 0).astype(jnp.bfloat16)
        line_cross_copy().start()
        line_kept[...] = jnp.concatenate(rows[: 2 * spans], 0)
        lax.fori_loop(MIDDLE, steps, both, 0)
        line_cross_copy().wait_recv()
        total = line_kept[...] + line_cross[...].astype(jnp.float32)
        line_last[...] = total[spans:].astype(jnp.bfloat16)
        line_final_copy().start()
        moved_out[...] = total[:spans].astype(jnp.bfloat16)

    def land(k, _):
        final_copy(k).wait_recv()
        far_copy(k).wait_recv()
        a, r = lax.div(k, per), lax.rem(k, per)
        start = pl.multiple_of(r * rows_per, rows_per)
        for l in range(spans):
            moved_cache[a, l, pl.ds(start, rows_per), :] = final_in[k, l] + final_far[k, l]
        return 0

    def outer_sent(k, _):
        raw_copy(mate, 0, 0, k).wait_send()
        raw_copy(mate_aside, 1, 1, k).wait_send()
        return 0

    def inner_sent(k, _):
        raw_copy(aside, 0, 2, k).wait_send()
        far_copy(k).wait_send()
        cross_copy(k).wait_send()
        final_copy(k).wait_send()
        return 0

    @pl.when(inner)
    def _():
        lax.fori_loop(steps - LAG, steps, finish, 0)
        label_copy(aside, 0, 2).wait_send()
        line_copy(aside, 0, 2).wait_send()
        line_cross_copy().wait_send()
        line_final_copy().wait_send()
        lax.fori_loop(0, steps, inner_sent, 0)

    @pl.when(outer)
    def _():
        lax.fori_loop(0, steps, land, 0)
        label_copy(mate, 0, 0).wait_send()
        label_copy(mate_aside, 1, 1).wait_send()
        line_copy(mate, 0, 0).wait_send()
        line_copy(mate_aside, 1, 1).wait_send()
        line_final_copy().wait_recv()
        moved_out[...] = line_final[...]
        lax.fori_loop(0, steps, outer_sent, 0)


def body(
    hidden,
    token_qkv,
    self_cache,
    cross_kv,
    cache_len,
    finished,
    new_slot,
    out_proj,
    ln_gain,
    ln_bias,
    query_proj,
):
    count, cores = lax.axis_size("batch"), lax.axis_size("mp")
    spans, width = hidden.shape
    slots, local = self_cache.shape[2:]
    moves = len(DISTANCES)
    smem = pl.BlockSpec(memory_space=pltpu.SMEM)
    vmem = pl.BlockSpec(memory_space=pltpu.VMEM)
    away = pl.BlockSpec(memory_space=pl.ANY)
    bf16, f32 = jnp.bfloat16, jnp.float32
    operands = (
        cache_len,
        finished,
        new_slot,
        hidden,
        token_qkv,
        self_cache,
        ln_gain,
        ln_bias,
        cross_kv,
        out_proj,
        query_proj,
    )
    parcels = pltpu.VMEM((moves, 2, slots, local), bf16)
    tiles = pltpu.VMEM((moves, 16, local), bf16)
    dma = pltpu.SemaphoreType.DMA
    inputs = [pltpu.VMEM(array.shape, bf16) for array in (cross_kv, out_proj, query_proj)]
    parts = [pltpu.VMEM((8, width), f32), pltpu.VMEM((cores - 1, 8, width), f32)]
    steps = 2 * slots // ROWS
    if count == 2 * (REACH + 1):
        function, specs = relay_kernel, [away] * 8

        def blocks(*lead):
            return pltpu.VMEM(lead + (ROWS, local), bf16)

        small = [pltpu.SMEM((spans,), jnp.int32)] * 3 + [
            pltpu.VMEM(hidden.shape, bf16),
            pltpu.VMEM(token_qkv.shape, bf16),
            pltpu.VMEM(ln_gain.shape, f32),
            pltpu.VMEM(ln_bias.shape, f32),
        ]
        scratch = small + [pltpu.VMEM(self_cache.shape, bf16)] + inputs + [
            blocks(steps, spans),
            blocks(3, steps, spans),
            blocks(steps, 2 * spans),
            blocks(steps, spans),
            blocks(steps, spans),
            blocks(steps, spans),
            blocks(steps, spans),
            blocks(steps, spans),
            blocks(4 * spans, 4 * spans),
            pltpu.VMEM((8, 128), f32),
            pltpu.VMEM((3, 8, 128), f32),
            pltpu.VMEM((spans, local), bf16),
            pltpu.VMEM((3, spans, local), bf16),
            pltpu.VMEM((2 * spans, local), f32),
            pltpu.VMEM((2 * spans, local), bf16),
            pltpu.VMEM((2 * spans, local), bf16),
            pltpu.VMEM((spans, local), bf16),
            pltpu.VMEM((spans, local), bf16),
            *parts,
            dma((12,)),
            dma((2, steps)),
            dma((3, steps)),
            dma((6, steps)),
            dma((2,)),
            dma((3,)),
            dma((2,)),
            dma((3,)),
            dma((4,)),
            dma((2, cores - 1)),
        ]
    else:
        function, specs = kernel, [smem] * 3 + [vmem] * 5
        scratch = inputs + [
            pltpu.VMEM(self_cache.shape, bf16),
            parcels,
            parcels,
            tiles,
            tiles,
            tiles,
            tiles,
            *parts,
            dma((3,)),
            dma((2, moves)),
            dma((2, moves)),
            dma((2, moves)),
            dma((2, cores - 1)),
        ]
    return pl.pallas_call(
        functools.partial(function, count, cores),
        out_shape=(
            pltpu.VMEM(self_cache.shape, bf16),
            pltpu.VMEM((spans, local), bf16),
        ),
        in_specs=specs + [away] * 3,
        out_specs=(vmem, vmem),
        scratch_shapes=scratch,
        compiler_params=pltpu.CompilerParams(collective_id=0, has_side_effects=True),
    )(*operands)


def solution(mesh):
    placed = (
        P(("groups", "batch"), None),
        P(None, ("groups", "batch"), "mp"),
        P(None, ("groups", "batch"), None, "mp"),
        P(None, ("groups", "batch"), None, "mp"),
        P(("groups", "batch")),
        P(("groups", "batch")),
        P(("groups", "batch")),
        P("mp", None),
        P(),
        P(),
        P(None, "mp"),
    )
    return jax.shard_map(
        body,
        mesh=mesh,
        in_specs=placed,
        out_specs=(P(None, ("groups", "batch"), None, "mp"), P(("groups", "batch"), "mp")),
        check_vma=False,
    )
```
